768 devices in a mesh: gx: 32 (over y, z_lo), gy: 3 (over z_hi), gz: 8 (over x, core).
Axes of the slice: x: 4, y: 8, z: 12 (z_hi: 3, z_lo: 4; z = z_hi * 4 + z_lo), core: 2. Of those that a mesh axis runs over, the one named last changes fastest.
Arguments:
- positions: float32 [32, 3, 8, 3, 128], P('gx', 'gy', 'gz'), may hold values from 0 to 3
- features: bfloat16 [32, 3, 8, 128, 576], P('gx', 'gy', 'gz'), may hold values from -6 to 6
- species: int32 [32, 3, 8, 128], P('gx', 'gy', 'gz'), may hold values from 0 to 1
- neighbours: int32 [32, 3, 8, 12, 128], P('gx', 'gy', 'gz'), may hold values from 0 to 1855, as said below
- send_list: int32 [32, 3, 8, 64], P('gx', 'gy', 'gz'), may hold values from 0 to 127, as said below
- mix_weight: bfloat16 [3, 64, 64], replicated, may hold values from -0.75 to 0.75
- radial_in: float32 [8, 64], replicated, may hold values from -2 to 2
- radial_out: float32 [64, 192], replicated, may hold values from -3 to 3
- readout: float32 [2, 3, 64], replicated, may hold values from -0.1875 to 0.1875
Outputs:
- atom_energy: float32 [32, 3, 8, 128], P('gx', 'gy', 'gz')
- forces: float32 [32, 3, 8, 3, 128], P('gx', 'gy', 'gz')
- feature_grad: float32 [32, 3, 8, 128, 576], P('gx', 'gy', 'gz')
The draws below stay inside these ranges and needn't reach their ends.
Inputs may be any that keep to these rules, and one draw needn't show every extreme that they name: `neighbours`: an entry below 128 is an own atom; an entry 128 + b * 64 + s is slot s of direction b, and b is never 13. `send_list`: the 64 entries of one brick are distinct.
All inputs are finite; a program needn't handle non-finite values.
Results may differ from the reference program's by a relative error of at most 0.0038.
Values may be sent and summed in bfloat16 or wider, within the bound.
A program may use at most 32 MiB of HBM per device.

```python
import math
import jax
import jax.numpy as jnp
from jax import lax

C = 64
F = 576
HID = 64
NBASIS = 8
NEIGH = 12
ATOMS = 128
SEND = 64
NGX = 32
NGY = 3
NGZ = 8


def draw_neighbours(key, part):
    first, second, third = jax.random.split(key, 3)
    shape_all = (NGX, NGY, NGZ, NEIGH, ATOMS)
    own_ids = jax.random.randint(first, shape_all, 0, ATOMS)
    ghost_ids = jax.random.randint(second, shape_all, 0, 26 * SEND)
    ghost_ids = ghost_ids + SEND * (ghost_ids >= 13 * SEND).astype(jnp.int32) + ATOMS
    pick_ghost = jax.random.randint(third, shape_all, 0, 3) == 0
    return jnp.where(pick_ghost, ghost_ids, own_ids).astype(jnp.int32)


def draw_send_list(key, part):
    subkeys = jax.random.split(jax.random.fold_in(key, 7), NGX * NGY * NGZ)
    picked = jax.vmap(lambda subkey: jax.random.permutation(subkey, ATOMS)[:SEND])(subkeys)
    return picked.reshape(NGX, NGY, NGZ, SEND).astype(jnp.int32)


def touch_ends(values, key, low, largest):
    dims = values.shape
    place = [jax.random.randint(jax.random.fold_in(key, axis), (), 0, dims[axis]) for axis in range(len(dims))]
    values = values.at[tuple(place)].set(low)
    longest = dims.index(max(dims))
    place[longest] = (place[longest] + 1) % dims[longest]
    return values.at[tuple(place)].set(largest)


def block_scale(own_key, shape, cuts, least, high):
    def one(axis_at, blocks):
        heights = jax.random.uniform(jax.random.fold_in(jax.random.fold_in(own_key, 6), axis_at), (blocks,), jnp.float32, least / len(cuts), high / len(cuts))
        return jnp.repeat(jnp.exp(heights), shape[axis_at] // blocks).reshape((-1,) + (1,) * (len(shape) - axis_at - 1))

    gain = one(*cuts[0])
    for cut in cuts[1:]:
        gain = gain * one(*cut)
    return gain


def gaussian(own_key, shape, scale, most, cuts=(), kind=jnp.bfloat16):
    values = scale * jax.random.normal(own_key, shape, jnp.float32)
    if cuts:
        values = values * block_scale(own_key, shape, cuts, -0.22, 0.18)
    return jnp.clip(values, -most, most).astype(kind)


def setup_inputs(seed: int = 0) -> dict:
    key_of = jax.random.split(jax.random.key(seed), 10)
    return {
        "positions": jnp.clip(3.0 * jax.random.uniform(key_of[0], (NGX, NGY, NGZ, 3, ATOMS), jnp.float32) ** block_scale(key_of[0], (NGX, NGY, NGZ, 3, ATOMS), ((0, 32), (1, 3), (2, 8)), -0.2, 0.2), 0.0, 3.0),
        "features": gaussian(key_of[1], (NGX, NGY, NGZ, ATOMS, F), 1.0, 6.0, ((0, 32), (1, 3), (2, 8))),
        "species": touch_ends(jax.random.randint(key_of[2], (NGX, NGY, NGZ, ATOMS), 0, 2), jax.random.fold_in(key_of[2], 1), 0, 1).astype(jnp.int32),
        "neighbours": draw_neighbours(jax.random.fold_in(key_of[9], 71), 0),
        "send_list": draw_send_list(jax.random.fold_in(key_of[9], 71), 0),
        "mix_weight": gaussian(key_of[5], (3, C, C), C ** -0.5, 0.75),
        "radial_in": gaussian(key_of[6], (NBASIS, HID), NBASIS ** -0.5, 2.0, (), jnp.float32),
        "radial_out": gaussian(key_of[7], (HID, 3 * C), 4 ** -0.5, 3.0, (), jnp.float32),
        "readout": gaussian(key_of[8], (2, 3, C), (16 * C) ** -0.5, 0.1875, (), jnp.float32),
    }


EDGE = 3.0
HIGH = lax.Precision.HIGHEST
LEVELS = (0, 1, 1, 1, 2, 2, 2, 2, 2)
ROOT_THREE = math.sqrt(3.0)
ROOT_FIVE = math.sqrt(5.0)
ROOT_FIFTEEN = math.sqrt(15.0)

def harmonics(direction):
    comp_x, comp_y, comp_z = (direction[0], direction[1], direction[2])
    return jnp.stack([jnp.ones_like(comp_x), ROOT_THREE * comp_x, ROOT_THREE * comp_y, ROOT_THREE * comp_z, ROOT_FIFTEEN * comp_x * comp_y, ROOT_FIFTEEN * comp_y * comp_z, 0.5 * ROOT_FIVE * (2.0 * comp_z * comp_z - comp_x * comp_x - comp_y * comp_y), ROOT_FIFTEEN * comp_x * comp_z, 0.5 * ROOT_FIFTEEN * (comp_x * comp_x - comp_y * comp_y)])

def geometry(displace, radial_in, radial_out):
    radius = jnp.sqrt(lax.optimization_barrier(jnp.sum(displace * displace, 0)) + 1.0)
    direction = displace / radius
    centres = 1.25 * jnp.arange(radial_in.shape[0]).astype(radius.dtype)
    spacing = radius[None, :] - centres[:, None]
    basis_set = jnp.exp(-0.5 * spacing * spacing)
    hidden = jax.nn.silu(jnp.dot(radial_in.T, basis_set, precision=HIGH))
    radial = lax.dot_general(hidden, radial_out, (((0,), (0,)), ((), ())), precision=HIGH)
    return (harmonics(direction), radial)

def spread(radial):
    atom_count = radial.shape[0]
    channels = radial.shape[1] // 3
    pieces = radial.reshape(atom_count, 3, channels)
    return jnp.concatenate([pieces[:, 0:1], jnp.broadcast_to(pieces[:, 1:2], (atom_count, 3, channels)), jnp.broadcast_to(pieces[:, 2:3], (atom_count, 5, channels))], 1)

def offsets():
    direction_id = jnp.arange(27)
    return EDGE * jnp.stack([direction_id // 9 - 1, direction_id // 3 % 3 - 1, direction_id % 3 - 1], 1).astype(jnp.float32)

def local_layer(table_g, table_pos, own_pos, species, neighbours, radial_in, radial_out, readout):
    atom_count = own_pos.shape[1]
    channels = table_g.shape[1] // 9
    norm_scale = 1.0 / math.sqrt(neighbours.shape[0])

    def fetch(slot_index):
        gathered = jnp.take(table_g, slot_index, axis=0).astype(jnp.float32).reshape(atom_count, 9, channels)
        displace = jnp.take(table_pos, slot_index, axis=1) - own_pos
        return (gathered, displace)

    def forward_step(running, slot_index):
        gathered, displace = fetch(slot_index)
        harmonic, radial = geometry(displace, radial_in, radial_out)
        radial_full = spread(radial)
        message = radial_full * (harmonic.T[:, :, None] * gathered[:, 0:1, :] + gathered)
        return (running + message, None)
    summed, _ = lax.scan(forward_step, jnp.zeros((atom_count, 9, channels), jnp.float32), neighbours)
    accum = summed * norm_scale
    weights = jnp.where(species[:, None, None] == 1, readout[1][None], readout[0][None])
    square_one = lax.optimization_barrier(jnp.sum(accum[:, 1:4] * accum[:, 1:4], 1))
    square_two = lax.optimization_barrier(jnp.sum(accum[:, 4:9] * accum[:, 4:9], 1))
    energy = lax.optimization_barrier(jnp.sum(weights[:, 0] * accum[:, 0] + weights[:, 1] * square_one + weights[:, 2] * square_two, -1))
    d_accum = jnp.concatenate([weights[:, 0:1], 2.0 * weights[:, 1:2] * accum[:, 1:4], 2.0 * weights[:, 2:3] * accum[:, 4:9]], 1) * norm_scale

    def backward_step(state_pair, slot_index):
        grad_g, grad_pos = state_pair
        gathered, displace = fetch(slot_index)
        (harmonic, radial), pullback = jax.vjp(lambda moved: geometry(moved, radial_in, radial_out), displace)
        radial_full = spread(radial)
        harmonic_t = harmonic.T[:, :, None]
        coupled = harmonic_t * gathered[:, 0:1, :] + gathered
        weighted = d_accum * radial_full
        d_rows = weighted.at[:, 0].add(lax.optimization_barrier(jnp.sum(weighted * harmonic_t, 1)))
        d_full = d_accum * coupled
        d_radial = jnp.concatenate([d_full[:, 0], lax.optimization_barrier(jnp.sum(d_full[:, 1:4], 1)), lax.optimization_barrier(jnp.sum(d_full[:, 4:9], 1))], 1)
        d_harmonic = lax.optimization_barrier(jnp.sum(weighted * gathered[:, 0:1, :], 2)).T
        d_displace, = pullback((d_harmonic, d_radial))
        grad_g = grad_g.at[slot_index].add(d_rows.reshape(atom_count, 9 * channels))
        grad_pos = grad_pos.at[:, slot_index].add(d_displace)
        grad_pos = grad_pos.at[:, :atom_count].add(-d_displace)
        return ((grad_g, grad_pos), None)
    rows_total = table_g.shape[0]
    start_pair = (jnp.zeros((rows_total, 9 * channels), jnp.float32), jnp.zeros((3, rows_total), jnp.float32))
    (grad_g, grad_pos), _ = lax.scan(backward_step, start_pair, neighbours)
    return (energy, grad_g, grad_pos)

def mixed_rows(own_feat, mix_weight):
    atom_count = own_feat.shape[0]
    channels = mix_weight.shape[1]
    expanded = mix_weight[jnp.array(LEVELS)].astype(jnp.float32)
    comps = own_feat.reshape(atom_count, 9, channels).astype(jnp.float32)
    result = jnp.einsum('amd,mde->ame', comps, expanded, precision=HIGH)
    return result.reshape(atom_count, 9 * channels).astype(jnp.bfloat16)

def reference(positions, features, species, neighbours, send_list, mix_weight, radial_in, radial_out, readout):
    size_x, size_y, size_z = (positions.shape[0], positions.shape[1], positions.shape[2])
    atom_count = positions.shape[4]
    width = features.shape[4]
    send_count = send_list.shape[3]
    bricks = size_x * size_y * size_z
    mixed = lax.map(lambda block: mixed_rows(block, mix_weight), features.reshape(bricks, atom_count, width))
    flat_send = send_list.reshape(bricks, send_count)
    buffer_g = jax.vmap(lambda block, picks: jnp.take(block, picks, axis=0))(mixed, flat_send)
    buffer_pos = jax.vmap(lambda block, picks: jnp.take(block, picks, axis=1))(positions.reshape(bricks, 3, atom_count), flat_send)
    buffer_g = buffer_g.reshape(size_x, size_y, size_z, send_count, width)
    buffer_pos = buffer_pos.reshape(size_x, size_y, size_z, 3, send_count)
    mixed = mixed.reshape(size_x, size_y, size_z, atom_count, width)
    shift_table = offsets()
    direction_id = jnp.arange(27)
    step_x = direction_id // 9 - 1
    step_y = direction_id // 3 % 3 - 1
    step_z = direction_id % 3 - 1

    def brick_step(state_pair, brick_id):
        return_g, return_pos = state_pair
        index_x = brick_id // (size_y * size_z)
        index_y = brick_id // size_z % size_y
        index_z = brick_id % size_z
        near_x = (index_x + step_x) % size_x
        near_y = (index_y + step_y) % size_y
        near_z = (index_z + step_z) % size_z
        ghost_g = buffer_g[near_x, near_y, near_z].reshape(27 * send_count, width)
        ghost_pos = buffer_pos[near_x, near_y, near_z] + shift_table[:, :, None]
        ghost_pos = jnp.transpose(ghost_pos, (1, 0, 2)).reshape(3, 27 * send_count)
        own_pos = positions[index_x, index_y, index_z]
        table_g = jnp.concatenate([mixed[index_x, index_y, index_z], ghost_g], 0)
        table_pos = jnp.concatenate([own_pos, ghost_pos], 1)
        energy, grad_g, grad_pos = local_layer(table_g, table_pos, own_pos, species[index_x, index_y, index_z], neighbours[index_x, index_y, index_z], radial_in, radial_out, readout)
        part_g = grad_g[atom_count:].reshape(27, send_count, width)
        part_pos = jnp.transpose(grad_pos[:, atom_count:].reshape(3, 27, send_count), (1, 0, 2))
        part_g = part_g.astype(jnp.bfloat16).astype(jnp.float32)
        part_pos = part_pos.astype(jnp.bfloat16).astype(jnp.float32)
        return_g = return_g.at[near_x, near_y, near_z].add(part_g)
        return_pos = return_pos.at[near_x, near_y, near_z].add(part_pos)
        return ((return_g, return_pos), (energy, grad_g[:atom_count], grad_pos[:, :atom_count]))
    start_pair = (jnp.zeros((size_x, size_y, size_z, send_count, width), jnp.float32), jnp.zeros((size_x, size_y, size_z, 3, send_count), jnp.float32))
    (return_g, return_pos), (energy, own_g, own_grad) = lax.scan(brick_step, start_pair, jnp.arange(bricks, dtype=jnp.int32))
    own_g = jax.vmap(lambda block, picks, extra: block.at[picks].add(extra))(own_g, flat_send, return_g.reshape(bricks, send_count, width))
    own_grad = jax.vmap(lambda block, picks, extra: block.at[:, picks].add(extra))(own_grad, flat_send, return_pos.reshape(bricks, 3, send_count))
    channels = mix_weight.shape[1]
    expanded = mix_weight[jnp.array(LEVELS)].astype(jnp.float32)
    feature_grad = lax.map(lambda block: jnp.einsum('ame,mde->amd', block.reshape(atom_count, 9, channels), expanded, precision=HIGH).reshape(atom_count, width), own_g)
    atom_energy = energy.reshape(size_x, size_y, size_z, atom_count)
    forces = -own_grad.reshape(size_x, size_y, size_z, 3, atom_count)
    return (atom_energy, forces, feature_grad.reshape(size_x, size_y, size_z, atom_count, width))
```

```python
import math

import jax
import jax.numpy as jnp
from jax import lax
from jax.experimental import pallas as pl
from jax.experimental.pallas import tpu as pltpu
from jax.sharding import PartitionSpec as P

EDGE = 3.0
HIGH = lax.Precision.HIGHEST
MESH = pl.DeviceIdType.MESH
LEVELS = (0, 1, 1, 1, 2, 2, 2, 2, 2)
ROOT_THREE = math.sqrt(3.0)
ROOT_FIVE = math.sqrt(5.0)
ROOT_FIFTEEN = math.sqrt(15.0)

ATOMS = 128
SEND = 64
SLOTS = 12
EDGES = SLOTS * ATOMS
CH = 64
FEAT = 576
WIDE = 640
FLAT0 = 128
PAIR0 = 640
ROWS = 1792

NN = (((1,), (0,)), ((), ()))
NT = (((1,), (1,)), ((), ()))
TN = (((0,), (0,)), ((), ()))
F32 = jnp.float32
BF16 = jnp.bfloat16


def dot(lhs, rhs, dims=NN, precision=None):
    return lax.dot_general(lhs, rhs, dims, precision=precision, preferred_element_type=F32)


def column(dx, dy):
    return (dx + 1) * 3 + dy + 1


def row_of(dx, dy, dz):
    spot = column(dx, dy)
    if dz == 0:
        return FLAT0 + SEND * (spot - (spot > 4))
    return PAIR0 + 2 * SEND * spot + SEND * (dz > 0)


def code(dx, dy, dz):
    return column(dx, dy) * 3 + dz + 1


def eye(size):
    return jnp.where(
        lax.broadcasted_iota(jnp.int32, (size, size), 0)
        == lax.broadcasted_iota(jnp.int32, (size, size), 1),
        1.0,
        0.0,
    ).astype(BF16)


def parts(value):
    first = value.astype(BF16).astype(F32)
    rest = value - first
    second = rest.astype(BF16).astype(F32)
    third = rest - second
    filler = jnp.zeros((40, value.shape[1]), F32)
    return jnp.concatenate([first, second, third, filler], 0).astype(BF16)


def split(value):
    high = value.astype(BF16)
    return high, (value - high.astype(F32)).astype(BF16)


def mixers(mix_ref):
    zero = jnp.zeros((CH, CH), BF16)

    def pair(upper, lower):
        return jnp.concatenate(
            [
                jnp.concatenate([mix_ref[upper], zero], 1),
                jnp.concatenate([zero, mix_ref[lower]], 1),
            ],
            0,
        )

    last = pair(2, 2)
    return (pair(0, 1), pair(1, 1), last, last)


def kernel(
    pos_ref,
    feat_ref,
    spec_ref,
    nbr_ref,
    list_ref,
    mix_ref,
    rin_ref,
    rout_ref,
    read_ref,
    energy_ref,
    force_ref,
    fgrad_ref,
    tbl,
    tbl_t,
    shared,
    onehot,
    gath,
    placed,
    base,
    index,
    radial,
    pre,
    harm,
    accum,
    drows,
    dlow,
    drad,
    dharm,
    acc0,
    zsend,
    zrecv,
    xsend,
    xrecv,
    ysend,
    yrecv,
    fsend_sem,
    frecv_sem,
    bsend_sem,
    brecv_sem,
):
    size_x, size_y, size_z = (lax.axis_size(name) for name in ("gx", "gy", "gz"))
    me_x, me_y, me_z = (lax.axis_index(name) for name in ("gx", "gy", "gz"))

    def device(dx, dy, dz):
        return (
            lax.rem(me_x + dx + size_x, size_x),
            lax.rem(me_y + dy + size_y, size_y),
            lax.rem(me_z + dz + size_z, size_z),
        )

    sides = ((0, -1, 0), (0, 1, 0), (-1, 0, 0), (1, 0, 0), (0, 0, -1), (0, 0, 1))
    barrier = pltpu.get_barrier_semaphore()
    for side in sides:
        pl.semaphore_signal(barrier, inc=1, device_id=device(*side), device_id_type=MESH)

    mix = mixers(mix_ref)
    eye_big = eye(ATOMS)
    pos8 = jnp.concatenate([pos_ref[...], jnp.zeros((5, ATOMS), F32)], 0)
    pos_parts = parts(pos8)
    for tile in range(4):
        lanes = slice(128 * tile, 128 * tile + 128)
        tbl[0:ATOMS, lanes] = dot(feat_ref[:, lanes], mix[tile]).astype(BF16)
    tbl[0:ATOMS, 512:FEAT] = dot(feat_ref[:, 512:FEAT], mix_ref[2]).astype(BF16)
    tbl[0:ATOMS, FEAT:WIDE] = dot(eye_big, pos_parts, NT).astype(BF16)
    picks_t = jnp.where(
        lax.broadcasted_iota(jnp.int32, (ATOMS, SEND), 0) == list_ref[...], 1.0, 0.0
    ).astype(BF16)
    picks = dot(eye(SEND), picks_t, NT).astype(BF16)
    shared[...] = dot(picks, tbl[0:ATOMS, :]).astype(BF16)

    pl.semaphore_wait(barrier, len(sides))

    def halo(dx, dy, dz, axis):
        go = [0, 0, 0]
        go[axis] = -(dx, dy, dz)[axis]
        from_ = [dx, dy, dz]
        from_[axis] = 0
        source = shared
        if any(from_):
            source = tbl.at[pl.ds(row_of(*from_), SEND), :]
        which = code(dx, dy, dz)
        return pltpu.make_async_remote_copy(
            src_ref=source,
            dst_ref=tbl.at[pl.ds(row_of(dx, dy, dz), SEND), :],
            send_sem=fsend_sem.at[which],
            recv_sem=frecv_sem.at[which],
            device_id=device(*go),
            device_id_type=MESH,
        )

    started = []

    def start(copy):
        copy.start()
        started.append(copy)

    for dy in (-1, 1):
        start(halo(0, dy, 0, 1))
    for dx in (-1, 1):
        start(halo(dx, 0, 0, 0))
    for dz in (-1, 1):
        start(halo(0, 0, dz, 2))

    near = nbr_ref[...]
    ghost = near - ATOMS
    block = ghost >> 6
    inside = ghost & 63
    step_x = (block * 57) >> 9
    line = (block * 43) >> 7
    step_y = line - 3 * step_x
    step_z = block - 3 * line
    spot = 3 * step_x + step_y
    flat = FLAT0 + SEND * (spot - jnp.where(spot > 4, 1, 0)) + inside
    paired = PAIR0 + 2 * SEND * spot + jnp.where(step_z > 1, SEND, 0) + inside
    own = near < ATOMS
    index[...] = jnp.where(own, near, jnp.where(step_z == 1, flat, paired))
    shifts = [
        jnp.where(own, 0.0, EDGE * (step - 1).astype(F32)) for step in (step_x, step_y, step_z)
    ]
    for slot in range(SLOTS):
        lanes = slice(128 * slot, 128 * slot + 128)
        base[:, lanes] = (
            jnp.concatenate([each[slot : slot + 1] for each in shifts] + [jnp.zeros((5, ATOMS), F32)], 0)
            - pos8
        )

    rows_iota = lax.broadcasted_iota(jnp.int32, (ATOMS, ATOMS), 0)

    def fill(slot, carry):
        lanes = pl.ds(pl.multiple_of(slot * ATOMS, ATOMS), ATOMS)
        wanted = index[pl.ds(slot, 1), :]
        for part in range(ROWS // ATOMS):
            onehot[part * ATOMS : (part + 1) * ATOMS, lanes] = jnp.where(
                rows_iota == wanted - part * ATOMS, 1.0, 0.0
            ).astype(BF16)
        return carry

    lax.fori_loop(0, SLOTS, fill, 0)

    def flip(row):
        for tile in range(5):
            lanes = slice(128 * tile, 128 * tile + 128)
            tbl_t[lanes, row : row + ATOMS] = dot(
                eye_big, tbl[row : row + ATOMS, lanes], NT
            ).astype(BF16)

    flip(0)

    for dy in (-1, 1):
        halo(0, dy, 0, 1).wait_recv()
        for dx in (-1, 1):
            start(halo(dx, dy, 0, 0))
        for dz in (-1, 1):
            start(halo(0, dy, dz, 2))
    for dy in (0, -1, 1):
        for dx in (-1, 1):
            halo(dx, dy, 0, 0).wait_recv()
            for dz in (-1, 1):
                start(halo(dx, dy, dz, 2))
    for pair in range(4):
        flip(FLAT0 + ATOMS * pair)
    for dx, dy in ((0, 0), (0, -1), (0, 1), (-1, 0), (1, 0), (-1, -1), (1, -1), (-1, 1), (1, 1)):
        for dz in (-1, 1):
            halo(dx, dy, dz, 2).wait_recv()
        flip(row_of(dx, dy, -1))
    for copy in started:
        copy.wait_send()

    def gather(step, carry):
        lanes = pl.ds(pl.multiple_of(step * 256, 256), 256)
        rows = dot(tbl_t[...], onehot[:, lanes])
        gath[:, lanes] = rows[0:FEAT].astype(BF16)
        placed[:, lanes] = rows[FEAT : FEAT + 8] + rows[FEAT + 8 : FEAT + 16] + rows[FEAT + 16 : FEAT + 24]
        return carry

    lax.fori_loop(0, EDGES // 256, gather, 0)

    displace = placed[...] + base[...]
    comp = [displace[axis : axis + 1] for axis in range(3)]
    radius = jnp.sqrt(comp[0] * comp[0] + comp[1] * comp[1] + comp[2] * comp[2] + 1.0)
    inverse = 1.0 / radius
    ux, uy, uz = (each * inverse for each in comp)
    harm[0:8, :] = jnp.concatenate(
        [
            ROOT_THREE * ux,
            ROOT_THREE * uy,
            ROOT_THREE * uz,
            ROOT_FIFTEEN * ux * uy,
            ROOT_FIFTEEN * uy * uz,
            0.5 * ROOT_FIVE * (2.0 * uz * uz - ux * ux - uy * uy),
            ROOT_FIFTEEN * ux * uz,
            0.5 * ROOT_FIFTEEN * (ux * ux - uy * uy),
        ],
        0,
    )
    spacing = radius - 1.25 * lax.broadcasted_iota(jnp.int32, (8, EDGES), 0).astype(F32)
    basis = jnp.exp(-0.5 * spacing * spacing)
    before = dot(rin_ref[...], basis, TN, HIGH)
    pre[...] = before
    hidden = before / (1.0 + jnp.exp(-before))
    radial[...] = dot(rout_ref[...], hidden, TN, HIGH)

    accum[...] = jnp.zeros((FEAT, ATOMS), F32)

    def forward(slot, carry):
        lanes = pl.ds(pl.multiple_of(slot * ATOMS, ATOMS), ATOMS)
        for part in range(4):
            low = 16 * part
            first = gath[low : low + 16, lanes].astype(F32)
            for m in range(9):
                rows = slice(CH * m + low, CH * m + low + 16)
                weight = radial[CH * LEVELS[m] + low : CH * LEVELS[m] + low + 16, lanes]
                if m == 0:
                    value = first + first
                else:
                    value = harm[m - 1 : m, lanes] * first + gath[rows, lanes].astype(F32)
                accum[rows, :] += weight * value
        return carry

    lax.fori_loop(0, SLOTS, forward, 0)

    norm = 1.0 / math.sqrt(SLOTS)
    kinds = (spec_ref[...] == 1).astype(F32)
    sheet = jnp.concatenate([read_ref[0], read_ref[1]], 0)
    level_row = lax.broadcasted_iota(jnp.int32, (6, ATOMS), 0)
    energy = jnp.zeros((1, ATOMS), F32)
    for level in range(3):
        chosen = jnp.where(level_row == level, 1.0 - kinds, 0.0) + jnp.where(
            level_row == level + 3, kinds, 0.0
        )
        weight = dot(sheet, chosen, TN, HIGH)
        total = jnp.zeros((CH, ATOMS), F32)
        for m in range(9):
            if LEVELS[m] != level:
                continue
            rows = slice(CH * m, CH * m + CH)
            value = accum[rows, :] * norm
            if level == 0:
                total = value
                accum[rows, :] = weight * norm
            else:
                total = total + value * value
                accum[rows, :] = (2.0 * norm) * weight * value
        energy = energy + jnp.sum(weight * total, 0, keepdims=True)
    energy_ref[...] = energy

    def backward(slot, carry):
        lanes = pl.ds(pl.multiple_of(slot * ATOMS, ATOMS), ATOMS)
        turns = [None] * 9
        for part in range(4):
            low = 16 * part
            first = gath[low : low + 16, lanes].astype(F32)
            weights = [radial[CH * l + low : CH * l + low + 16, lanes] for l in range(3)]
            slope = accum[low : low + 16, :]
            grad_first = 2.0 * (slope * weights[0])
            grad_radial = [2.0 * (slope * first), None, None]
            for m in range(1, 9):
                level = LEVELS[m]
                rows = slice(CH * m + low, CH * m + low + 16)
                slope = accum[rows, :]
                turn = harm[m - 1 : m, lanes]
                weighted = slope * weights[level]
                high, rest = split(weighted)
                drows[rows, lanes] = high
                dlow[rows, lanes] = rest
                grad_first = grad_first + weighted * turn
                term = slope * (turn * first + gath[rows, lanes].astype(F32))
                grad_radial[level] = term if grad_radial[level] is None else grad_radial[level] + term
                spin = weighted * first
                turns[m] = spin if turns[m] is None else turns[m] + spin
            high, rest = split(grad_first)
            drows[low : low + 16, lanes] = high
            dlow[low : low + 16, lanes] = rest
            for level in range(3):
                drad[CH * level + low : CH * level + low + 16, lanes] = grad_radial[level]
        dharm[:, lanes] = jnp.concatenate(
            [jnp.sum(turns[m], 0, keepdims=True) for m in range(1, 9)], 0
        )
        return carry

    lax.fori_loop(0, SLOTS, backward, 0)

    before = pre[...]
    sigmoid = 1.0 / (1.0 + jnp.exp(-before))
    grad_hidden = dot(rout_ref[...], drad[...], NN, HIGH)
    grad_before = grad_hidden * (sigmoid * (1.0 + before * (1.0 - sigmoid)))
    grad_basis = dot(rin_ref[...], grad_before, NN, HIGH)
    grad_radius = jnp.sum(-(grad_basis * basis * spacing), 0, keepdims=True)
    dy1, dy2, dy3, dy4, dy5, dy6, dy7, dy8 = (dharm[m : m + 1, :] for m in range(8))
    grad_ux = ROOT_THREE * dy1 + ROOT_FIFTEEN * (uy * dy4 + uz * dy7 + ux * dy8) - ROOT_FIVE * ux * dy6
    grad_uy = ROOT_THREE * dy2 + ROOT_FIFTEEN * (ux * dy4 + uz * dy5 - uy * dy8) - ROOT_FIVE * uy * dy6
    grad_uz = ROOT_THREE * dy3 + ROOT_FIFTEEN * (uy * dy5 + ux * dy7) + 2.0 * ROOT_FIVE * uz * dy6
    along = ux * grad_ux + uy * grad_uy + uz * grad_uz
    grad_displace = jnp.concatenate(
        [
            (grad - unit * along) * inverse + grad_radius * unit
            for grad, unit in ((grad_ux, ux), (grad_uy, uy), (grad_uz, uz))
        ]
        + [jnp.zeros((5, EDGES), F32)],
        0,
    )
    drows[FEAT:WIDE, :] = parts(grad_displace)
    dlow[FEAT:WIDE, :] = jnp.zeros((WIDE - FEAT, EDGES), BF16)
    moved = grad_displace[:, 0:ATOMS]
    for slot in range(1, SLOTS):
        moved = moved + grad_displace[:, ATOMS * slot : ATOMS * slot + ATOMS]

    def back(source, target, which, go):
        return pltpu.make_async_remote_copy(
            src_ref=source,
            dst_ref=target,
            send_sem=bsend_sem.at[which],
            recv_sem=brecv_sem.at[which],
            device_id=device(*go),
            device_id_type=MESH,
        )

    def back_z(dx, dy, dz):
        where = pl.ds(row_of(dx, dy, dz) - PAIR0, SEND)
        return back(zsend.at[where, :], zrecv.at[where, :], code(dx, dy, dz), (0, 0, dz))

    def back_x(dx, dy):
        which = 3 * (dx > 0) + dy + 1
        return back(xsend.at[which], xrecv.at[which], code(dx, dy, 0), (dx, 0, 0))

    def back_y(dy):
        which = 1 * (dy > 0)
        return back(ysend.at[which], yrecv.at[which], code(0, dy, 0), (0, dy, 0))

    sent = []

    def send(copy):
        copy.start()
        sent.append(copy)

    for dx in (-1, 1, 0):
        row = row_of(dx, -1, -1)
        zsend[row - PAIR0 : row - PAIR0 + 384, :] = dot(
            onehot[row : row + 384, :], drows[...], NT
        ).astype(BF16)
        for dy in (-1, 1, 0):
            for dz in (-1, 1):
                send(back_z(dx, dy, dz))
    acc0[...] = dot(onehot[0:PAIR0, :], drows[...], NT)
    acc0[0:ATOMS, :] += dot(onehot[0:ATOMS, :], dlow[...], NT)

    def arrived_z(dx, dy):
        total = None
        for dz in (-1, 1):
            back_z(dx, dy, dz).wait_recv()
            row = row_of(dx, dy, dz) - PAIR0
            value = zrecv[row : row + SEND, :].astype(F32)
            total = value if total is None else total + value
        if (dx, dy) == (0, 0):
            return total
        row = row_of(dx, dy, 0)
        return total + acc0[row : row + SEND, :]

    for dy in (-1, 1, 0):
        for dx in (-1, 1):
            xsend[3 * (dx > 0) + dy + 1] = arrived_z(dx, dy).astype(BF16)
            send(back_x(dx, dy))
    totals = []
    for dy in (-1, 1, 0):
        total = arrived_z(0, dy)
        for dx in (-1, 1):
            back_x(dx, dy).wait_recv()
            total = total + xrecv[3 * (dx > 0) + dy + 1].astype(F32)
        if dy:
            ysend[1 * (dy > 0)] = total.astype(BF16)
            send(back_y(dy))
    for dy in (-1, 1):
        back_y(dy).wait_recv()
        total = total + yrecv[1 * (dy > 0)].astype(F32)
    high, rest = split(total)
    owned = acc0[0:ATOMS, :] + dot(picks_t, high) + dot(picks_t, rest)
    for tile in range(4):
        lanes = slice(128 * tile, 128 * tile + 128)
        high, rest = split(owned[:, lanes])
        fgrad_ref[:, lanes] = dot(high, mix[tile], NT) + dot(rest, mix[tile], NT)
    high, rest = split(owned[:, 512:FEAT])
    fgrad_ref[:, 512:FEAT] = dot(high, mix_ref[2], NT) + dot(rest, mix_ref[2], NT)
    turned = dot(eye(SEND).astype(F32), owned[:, FEAT:WIDE], NT, HIGH)
    force = moved - (turned[0:8] + turned[8:16] + turned[16:24])
    force_ref[...] = force[0:3]
    for copy in sent:
        copy.wait_send()


def shards(
    positions, features, species, neighbours, send_list, mix_weight, radial_in, radial_out, readout
):
    vmem = pl.BlockSpec(memory_space=pltpu.VMEM)
    energy, forces, feature_grad = pl.pallas_call(
        kernel,
        out_shape=(
            jax.ShapeDtypeStruct((1, ATOMS), F32),
            jax.ShapeDtypeStruct((3, ATOMS), F32),
            jax.ShapeDtypeStruct((ATOMS, FEAT), F32),
        ),
        in_specs=[vmem] * 9,
        out_specs=(vmem, vmem, vmem),
        scratch_shapes=[
            pltpu.VMEM((ROWS, WIDE), BF16),
            pltpu.VMEM((WIDE, ROWS), BF16),
            pltpu.VMEM((SEND, WIDE), BF16),
            pltpu.VMEM((ROWS, EDGES), BF16),
            pltpu.VMEM((FEAT, EDGES), BF16),
            pltpu.VMEM((8, EDGES), F32),
            pltpu.VMEM((8, EDGES), F32),
            pltpu.VMEM((SLOTS, ATOMS), jnp.int32),
            pltpu.VMEM((3 * CH, EDGES), F32),
            pltpu.VMEM((CH, EDGES), F32),
            pltpu.VMEM((8, EDGES), F32),
            pltpu.VMEM((FEAT, ATOMS), F32),
            pltpu.VMEM((WIDE, EDGES), BF16),
            pltpu.VMEM((WIDE, EDGES), BF16),
            pltpu.VMEM((3 * CH, EDGES), F32),
            pltpu.VMEM((8, EDGES), F32),
            pltpu.VMEM((PAIR0, WIDE), F32),
            pltpu.VMEM((ROWS - PAIR0, WIDE), BF16),
            pltpu.VMEM((ROWS - PAIR0, WIDE), BF16),
            pltpu.VMEM((6, SEND, WIDE), BF16),
            pltpu.VMEM((6, SEND, WIDE), BF16),
            pltpu.VMEM((2, SEND, WIDE), BF16),
            pltpu.VMEM((2, SEND, WIDE), BF16),
            pltpu.SemaphoreType.DMA((27,)),
            pltpu.SemaphoreType.DMA((27,)),
            pltpu.SemaphoreType.DMA((27,)),
            pltpu.SemaphoreType.DMA((27,)),
        ],
        compiler_params=pltpu.CompilerParams(
            collective_id=0, has_side_effects=True, vmem_limit_bytes=60 * 1024 * 1024
        ),
        name="layer",
    )(
        positions[0, 0, 0],
        features[0, 0, 0],
        species[0, 0],
        neighbours[0, 0, 0],
        send_list[0, 0],
        mix_weight,
        radial_in,
        radial_out,
        readout,
    )
    return (energy[None, None], forces[None, None, None], feature_grad[None, None, None])


def solution(mesh):
    in_specs = (
        P("gx", "gy", "gz", None, None),
        P("gx", "gy", "gz", None, None),
        P("gx", "gy", "gz", None),
        P("gx", "gy", "gz", None, None),
        P("gx", "gy", "gz", None),
        P(),
        P(),
        P(),
        P(),
    )
    out_specs = (
        P("gx", "gy", "gz", None),
        P("gx", "gy", "gz", None, None),
        P("gx", "gy", "gz", None, None),
    )
    return jax.shard_map(shards, mesh=mesh, in_specs=in_specs, out_specs=out_specs, check_vma=False)
```

```python
import math

import jax
import jax.numpy as jnp
from jax import lax
from jax.experimental import pallas as pl
from jax.experimental.pallas import tpu as pltpu
from jax.sharding import PartitionSpec as P

EDGE = 3.0
HIGH = lax.Precision.HIGHEST
MESH = pl.DeviceIdType.MESH
LEVELS = (0, 1, 1, 1, 2, 2, 2, 2, 2)
ROOT_THREE = math.sqrt(3.0)
ROOT_FIVE = math.sqrt(5.0)
ROOT_FIFTEEN = math.sqrt(15.0)

ATOMS = 128
SEND = 64
SLOTS = 12
EDGES = SLOTS * ATOMS
CH = 64
FEAT = 576
HALF = 288
RUN = 4

ORDER = ((0, -1), (0, 1), (-1, 0), (1, 0), (-1, -1), (1, -1), (-1, 1), (1, 1))
FLAT0 = 256
PAIR0 = 768
ROWS = 1792
BLOCKS = ROWS // SEND

NN = (((1,), (0,)), ((), ()))
NT = (((1,), (1,)), ((), ()))
TN = (((0,), (0,)), ((), ()))
F32 = jnp.float32
BF16 = jnp.bfloat16


def dot(lhs, rhs, dims=NN, precision=None):
    return lax.dot_general(lhs, rhs, dims, precision=precision, preferred_element_type=F32)


def column(dx, dy):
    return (dx + 1) * 3 + dy + 1


def slot_of(dx, dy, dz):
    if (dx, dy) == (0, 0):
        return 2 + (dz > 0)
    rank = ORDER.index((dx, dy))
    if dz == 0:
        return FLAT0 // SEND + rank
    return PAIR0 // SEND + 2 * rank + (dz > 0)


def parts(value):
    first = value[0:3].astype(BF16).astype(F32)
    rest = value[0:3] - first
    second = rest.astype(BF16).astype(F32)
    filler = jnp.zeros((7, value.shape[1]), F32)
    return jnp.concatenate([first, second, rest - second, filler], 0)


def joined(rows):
    total = rows[0:3] + rows[3:6] + rows[6:9]
    return jnp.concatenate([total, jnp.zeros((5, rows.shape[1]), F32)], 0)


def split(value):
    high = value.astype(BF16)
    return high, (value - high.astype(F32)).astype(BF16)


def mixers(mix_ref):
    zero = jnp.zeros((CH, CH), BF16)

    def pair(upper, lower):
        return jnp.concatenate(
            [
                jnp.concatenate([mix_ref[upper], zero], 1),
                jnp.concatenate([zero, mix_ref[lower]], 1),
            ],
            0,
        )

    last = pair(2, 2)
    return (pair(0, 1), pair(1, 1), last, last)


def kernel(
    pos_ref,
    feat_ref,
    spec_ref,
    nbr_ref,
    list_ref,
    mix_ref,
    rin_ref,
    rout_ref,
    read_ref,
    energy_ref,
    force_ref,
    fgrad_ref,
    shared,
    ghosts,
    place,
    tbl,
    prows,
    onehot,
    inner,
    blocks,
    total_g,
    gath,
    placed,
    base,
    index,
    radial,
    pre,
    harm,
    basis_ref,
    accum,
    drows,
    dlow,
    drad,
    dharm,
    masked,
    own_g,
    flat_g,
    zsend,
    zrecv,
    xsend,
    xrecv,
    ysend,
    yrecv,
    pgrad,
    pzrecv,
    pxsend,
    pxrecv,
    pysend,
    pyrecv,
    fsend_sem,
    frecv_sem,
    bsend_sem,
    brecv_sem,
    psend_sem,
    precv_sem,
):
    size_x, size_y, size_z = (lax.axis_size(name) for name in ("gx", "gy", "gz"))
    me_x, me_y, me_z = (lax.axis_index(name) for name in ("gx", "gy", "gz"))
    run_at = lax.rem(me_x, RUN)
    bend = {-1: -jnp.where(run_at == 0, 1, 0), 1: jnp.where(run_at == RUN - 1, 1, 0)}

    def device(dx, dy, dz):
        turn = bend[dx] if dx else 0
        return (
            lax.rem(me_x + dx + size_x, size_x),
            lax.rem(me_y + dy + turn + size_y, size_y),
            lax.rem(me_z + dz + size_z, size_z),
        )

    sides = ((0, -1, 0), (0, 1, 0), (-1, 0, 0), (1, 0, 0), (0, 0, -1), (0, 0, 1))
    barrier = pltpu.get_barrier_semaphore()
    for side in sides:
        pl.semaphore_signal(barrier, inc=1, device_id=device(*side), device_id_type=MESH)

    mix = mixers(mix_ref)
    pos8 = jnp.concatenate([pos_ref[0], pos_ref[1], pos_ref[2], jnp.zeros((5, ATOMS), F32)], 0)
    for tile in range(4):
        rows = slice(128 * tile, 128 * tile + 128)
        tbl[rows, 0:ATOMS] = dot(mix[tile], feat_ref[rows, :], TN).astype(BF16)
    tbl[512:FEAT, 0:ATOMS] = dot(mix_ref[2], feat_ref[512:FEAT, :], TN).astype(BF16)
    picks = jnp.where(
        lax.broadcasted_iota(jnp.int32, (ATOMS, SEND), 0) == list_ref[...], 1.0, 0.0
    ).astype(BF16)
    zero = jnp.zeros((ATOMS, SEND), BF16)
    picks_left = jnp.concatenate([picks, zero], 1)
    picks_right = jnp.concatenate([zero, picks], 1)
    shared[...] = (
        dot(tbl[0:HALF, 0:ATOMS], picks_left) + dot(tbl[HALF:FEAT, 0:ATOMS], picks_right)
    ).astype(BF16)
    pos_parts = parts(pos8).astype(BF16)
    place[0, 4] = joined(dot(pos_parts, picks_left))

    pl.semaphore_wait(barrier, len(sides))

    started = []

    def start(copy):
        copy.start()
        started.append(copy)

    def remote(source, target, sends, recvs, which, go):
        return pltpu.make_async_remote_copy(
            src_ref=source,
            dst_ref=target,
            send_sem=sends.at[which],
            recv_sem=recvs.at[which],
            device_id=device(*go),
            device_id_type=MESH,
        )

    def halo(dx, dy, dz, axis):
        go = [0, 0, 0]
        go[axis] = -(dx, dy, dz)[axis]
        origin = [dx, dy, dz]
        origin[axis] = 0
        source = ghosts.at[slot_of(*origin)] if any(origin) else shared
        which = slot_of(dx, dy, dz)
        return remote(source, ghosts.at[which], fsend_sem, frecv_sem, which, go)

    def halo_place(axis, side):
        which = 2 * axis + (side > 0)
        if axis == 1:
            source, target, go = place.at[0, 4], place.at[0, 4 + side], (0, -side, 0)
        elif axis == 0:
            source, target = place.at[0, pl.ds(3, 3)], place.at[0, pl.ds(3 + 3 * side, 3)]
            go = (-side, 0, 0)
        else:
            source, target, go = place.at[0], place.at[1 + (side > 0)], (0, 0, -side)
        return remote(source, target, psend_sem, precv_sem, which, go)

    for side in (-1, 1):
        start(halo_place(1, side))
    for dy in (-1, 1):
        start(halo(0, dy, 0, 1))
    for dx in (-1, 1):
        start(halo(dx, 0, 0, 0))
    for dz in (-1, 1):
        start(halo(0, 0, dz, 2))

    near = jnp.concatenate([nbr_ref[slot] for slot in range(SLOTS)], 0)
    ghost = near - ATOMS
    block = ghost >> 6
    step_x = (block * 57) >> 9
    line = (block * 43) >> 7
    step_y = line - 3 * step_x
    step_z = block - 3 * line
    through = step_y - jnp.where(step_x == 0, bend[-1], jnp.where(step_x == 2, bend[1], 0))
    through = jnp.where(through < 0, through + 3, jnp.where(through > 2, through - 3, through))
    spot = 3 * step_x + through
    flat = jnp.zeros_like(spot)
    paired = jnp.full_like(spot, ATOMS)
    for rank, (dx, dy) in enumerate(ORDER):
        here = spot == column(dx, dy)
        flat = jnp.where(here, FLAT0 + SEND * rank, flat)
        paired = jnp.where(here, PAIR0 + 2 * SEND * rank, paired)
    paired = paired + jnp.where(step_z > 1, SEND, 0)
    own = near < ATOMS
    row = jnp.where(own, near, jnp.where(step_z == 1, flat, paired) + (ghost & 63))
    index[...] = row
    shifts = [
        jnp.where(own, 0.0, EDGE * (step - 1).astype(F32)) for step in (step_x, step_y, step_z)
    ]
    for slot in range(SLOTS):
        lanes = slice(128 * slot, 128 * slot + 128)
        blocks[0:1, lanes] = row[slot : slot + 1] >> 6
        base[:, lanes] = (
            jnp.concatenate([each[slot : slot + 1] for each in shifts] + [jnp.zeros((5, ATOMS), F32)], 0)
            - pos8
        )

    rows_iota = lax.broadcasted_iota(jnp.int32, (ATOMS, ATOMS), 0)

    def fill(slot, carry):
        lanes = pl.ds(pl.multiple_of(slot * ATOMS, ATOMS), ATOMS)
        wanted = index[pl.ds(slot, 1), :]
        inner[:, lanes] = jnp.where(rows_iota[0:SEND] == (wanted & 63), 1.0, 0.0).astype(BF16)
        for part in range(ROWS // ATOMS):
            onehot[part * ATOMS : (part + 1) * ATOMS, lanes] = jnp.where(
                rows_iota == wanted - part * ATOMS, 1.0, 0.0
            ).astype(BF16)
        return carry

    lax.fori_loop(0, SLOTS, fill, 0)

    def settle(row, left, right):
        lanes = slice(row, row + 128)
        for part in range(2):
            half = slice(SEND * part, SEND * part + SEND)
            tbl[HALF * part : HALF * part + HALF, lanes] = jnp.concatenate(
                [ghosts[left][:, half], ghosts[right][:, half]], 1
            )

    def settle_pair(dx, dy):
        left, right = slot_of(dx, dy, -1), slot_of(dx, dy, 1)
        settle(SEND * left, left, right)

    def gather(low, high):
        def one(step, carry):
            lanes = pl.ds(pl.multiple_of(step * 256, 256), 256)
            rows = dot(tbl[:, low:high], onehot[low:high, lanes])
            if low:
                rows = rows + total_g[:, lanes]
            if high == ROWS:
                gath[:, lanes] = rows.astype(BF16)
            else:
                total_g[:, lanes] = rows
            return carry

        lax.fori_loop(0, EDGES // 256, one, 0)

    for side in (-1, 1):
        halo_place(1, side).wait_recv()
    for side in (-1, 1):
        start(halo_place(0, side))
    for dy in (-1, 1):
        halo(0, dy, 0, 1).wait_recv()
        for dx in (-1, 1):
            start(halo(dx, dy, 0, 0))
        for dz in (-1, 1):
            start(halo(0, dy, dz, 2))
    for side in (-1, 1):
        halo_place(0, side).wait_recv()
    for side in (-1, 1):
        start(halo_place(2, side))
    for dx in (-1, 1):
        halo(dx, 0, 0, 0).wait_recv()
        for dz in (-1, 1):
            start(halo(dx, 0, dz, 2))
    for dz in (-1, 1):
        halo(0, 0, dz, 2).wait_recv()
    settle_pair(0, 0)
    gather(0, FLAT0)
    for dy in (-1, 1):
        for dx in (-1, 1):
            halo(dx, dy, 0, 0).wait_recv()
            for dz in (-1, 1):
                start(halo(dx, dy, dz, 2))
    for rank in range(0, 8, 2):
        left = FLAT0 // SEND + rank
        settle(SEND * left, left, left + 1)
    gather(FLAT0, PAIR0)

    for side in (-1, 1):
        halo_place(2, side).wait_recv()
    for half in range(2):
        prows[16 * half : 16 * half + 16, 0:SEND] = pos_parts[:, SEND * half : SEND * half + SEND]
    for dx in (-1, 0, 1):
        for dy in (-1, 0, 1):
            for dz in (-1, 0, 1):
                if (dx, dy, dz) != (0, 0, 0):
                    slot = slot_of(dx, dy, dz)
                    prows[16 * slot : 16 * slot + 16, :] = parts(
                        place[0 if dz == 0 else 1 + (dz > 0), column(dx, dy)]
                    ).astype(BF16)

    def locate(step, carry):
        lanes = pl.ds(pl.multiple_of(step * 256, 256), 256)
        rows = dot(prows[:, 0:SEND], inner[:, lanes])
        where = blocks[0:1, lanes]
        chosen = jnp.zeros((16, 256), F32)
        for slot in range(BLOCKS):
            chosen = jnp.where(where == slot, rows[16 * slot : 16 * slot + 16], chosen)
        placed[:, lanes] = joined(chosen)
        return carry

    lax.fori_loop(0, EDGES // 256, locate, 0)
    displace = placed[...] + base[...]
    comp = [displace[axis : axis + 1] for axis in range(3)]
    radius = jnp.sqrt(comp[0] * comp[0] + comp[1] * comp[1] + comp[2] * comp[2] + 1.0)
    inverse = 1.0 / radius
    ux, uy, uz = (each * inverse for each in comp)
    harm[0:8, :] = jnp.concatenate(
        [
            ROOT_THREE * ux,
            ROOT_THREE * uy,
            ROOT_THREE * uz,
            ROOT_FIFTEEN * ux * uy,
            ROOT_FIFTEEN * uy * uz,
            0.5 * ROOT_FIVE * (2.0 * uz * uz - ux * ux - uy * uy),
            ROOT_FIFTEEN * ux * uz,
            0.5 * ROOT_FIFTEEN * (ux * ux - uy * uy),
        ],
        0,
    )
    spacing = radius - 1.25 * lax.broadcasted_iota(jnp.int32, (8, EDGES), 0).astype(F32)
    basis = jnp.exp(-0.5 * spacing * spacing)
    basis_ref[...] = basis * spacing
    before = dot(rin_ref[...], basis, TN, HIGH)
    pre[...] = before
    hidden = before / (1.0 + jnp.exp(-before))
    radial[...] = dot(rout_ref[...], hidden, TN, HIGH)

    for dx, dy in ORDER[:4]:
        for dz in (-1, 1):
            halo(dx, dy, dz, 2).wait_recv()
        settle_pair(dx, dy)
    gather(PAIR0, PAIR0 + 512)
    for dx, dy in ORDER[4:]:
        for dz in (-1, 1):
            halo(dx, dy, dz, 2).wait_recv()
        settle_pair(dx, dy)
    gather(PAIR0 + 512, ROWS)

    accum[...] = jnp.zeros((FEAT, ATOMS), F32)

    def forward(slot, carry):
        lanes = pl.ds(pl.multiple_of(slot * ATOMS, ATOMS), ATOMS)
        for part in range(4):
            low = 16 * part
            first = gath[low : low + 16, lanes].astype(F32)
            for m in range(9):
                rows = slice(CH * m + low, CH * m + low + 16)
                weight = radial[CH * LEVELS[m] + low : CH * LEVELS[m] + low + 16, lanes]
                if m == 0:
                    value = first + first
                else:
                    value = harm[m - 1 : m, lanes] * first + gath[rows, lanes].astype(F32)
                accum[rows, :] += weight * value
        return carry

    lax.fori_loop(0, SLOTS, forward, 0)

    norm = 1.0 / math.sqrt(SLOTS)
    kinds = (spec_ref[...] == 1).astype(F32)
    by_kind = jnp.concatenate([1.0 - kinds, kinds], 0)
    energy = jnp.zeros((1, ATOMS), F32)
    for level in range(3):
        weight = dot(read_ref[level], by_kind, TN, HIGH)
        total = jnp.zeros((CH, ATOMS), F32)
        for m in range(9):
            if LEVELS[m] != level:
                continue
            rows = slice(CH * m, CH * m + CH)
            value = accum[rows, :] * norm
            if level == 0:
                total = value
                accum[rows, :] = weight * norm
            else:
                total = total + value * value
                accum[rows, :] = (2.0 * norm) * weight * value
        energy = energy + jnp.sum(weight * total, 0, keepdims=True)
    energy_ref[...] = energy

    def backward(slot, carry):
        lanes = pl.ds(pl.multiple_of(slot * ATOMS, ATOMS), ATOMS)
        turns = [None] * 9
        for part in range(4):
            low = 16 * part
            first = gath[low : low + 16, lanes].astype(F32)
            weights = [radial[CH * l + low : CH * l + low + 16, lanes] for l in range(3)]
            slope = accum[low : low + 16, :]
            grad_first = 2.0 * (slope * weights[0])
            grad_radial = [2.0 * (slope * first), None, None]
            for m in range(1, 9):
                level = LEVELS[m]
                rows = slice(CH * m + low, CH * m + low + 16)
                slope = accum[rows, :]
                turn = harm[m - 1 : m, lanes]
                weighted = slope * weights[level]
                high, rest = split(weighted)
                drows[rows, lanes] = high
                dlow[rows, lanes] = rest
                grad_first = grad_first + weighted * turn
                term = slope * (turn * first + gath[rows, lanes].astype(F32))
                grad_radial[level] = term if grad_radial[level] is None else grad_radial[level] + term
                spin = weighted * first
                turns[m] = spin if turns[m] is None else turns[m] + spin
            high, rest = split(grad_first)
            drows[low : low + 16, lanes] = high
            dlow[low : low + 16, lanes] = rest
            for level in range(3):
                drad[CH * level + low : CH * level + low + 16, lanes] = grad_radial[level]
        dharm[:, lanes] = jnp.concatenate(
            [jnp.sum(turns[m], 0, keepdims=True) for m in range(1, 9)], 0
        )
        return carry

    lax.fori_loop(0, SLOTS, backward, 0)

    def back_z(dx, dy, dz):
        which = slot_of(dx, dy, dz) - (2 if (dx, dy) == (0, 0) else PAIR0 // SEND - 2)
        return remote(
            zsend.at[which], zrecv.at[which], bsend_sem, brecv_sem, slot_of(dx, dy, dz), (0, 0, dz)
        )

    def back_x(dx, dy):
        which = 3 * (dx > 0) + dy + 1
        return remote(
            xsend.at[which], xrecv.at[which], bsend_sem, brecv_sem, slot_of(dx, dy, 0), (dx, 0, 0)
        )

    def back_y(dy):
        which = 1 * (dy > 0)
        return remote(
            ysend.at[which], yrecv.at[which], bsend_sem, brecv_sem, slot_of(0, dy, 0), (0, dy, 0)
        )

    def back_place(axis, side):
        at = 1 * (side > 0)
        if axis == 2:
            source, target, go = pgrad.at[1 + at], pzrecv.at[at], (0, 0, side)
        elif axis == 0:
            source, target, go = pxsend.at[at], pxrecv.at[at], (side, 0, 0)
        else:
            source, target, go = pysend.at[at], pyrecv.at[at], (0, side, 0)
        return remote(source, target, psend_sem, precv_sem, 6 + 2 * axis + at, go)

    def folded(pair):
        return [
            jnp.concatenate(
                [pair[0:HALF, SEND * part : SEND * part + SEND], pair[HALF:FEAT, SEND * part : SEND * part + SEND]],
                1,
            )
            for part in range(2)
        ]

    def send_pairs(row, columns):
        rows = dot(drows[...], onehot[row : row + 128 * len(columns), :], NT)
        for at, (dx, dy) in enumerate(columns):
            blocks_ = folded(rows[:, 128 * at : 128 * at + 128])
            for dz, value in zip((-1, 1), blocks_):
                which = slot_of(dx, dy, dz) - (2 if (dx, dy) == (0, 0) else PAIR0 // SEND - 2)
                zsend[which] = value.astype(BF16)
                start(back_z(dx, dy, dz))

    def keep_flats(rank):
        rows = dot(drows[...], onehot[FLAT0 + SEND * rank : FLAT0 + SEND * rank + 256, :], NT)
        for at in range(2):
            for part, value in enumerate(folded(rows[:, 128 * at : 128 * at + 128])):
                flat_g[rank + 2 * at + part] = value

    for rank in (4, 6, 2):
        send_pairs(PAIR0 + 128 * rank, ORDER[rank : rank + 2])

    before = pre[...]
    sigmoid = 1.0 / (1.0 + jnp.exp(-before))
    grad_hidden = dot(rout_ref[...], drad[...], NN, HIGH)
    grad_before = grad_hidden * (sigmoid * (1.0 + before * (1.0 - sigmoid)))
    grad_basis = dot(rin_ref[...], grad_before, NN, HIGH)
    grad_radius = jnp.sum(-(grad_basis * basis_ref[...]), 0, keepdims=True)
    displace = placed[...] + base[...]
    comp = [displace[axis : axis + 1] for axis in range(3)]
    radius = jnp.sqrt(comp[0] * comp[0] + comp[1] * comp[1] + comp[2] * comp[2] + 1.0)
    inverse = 1.0 / radius
    ux, uy, uz = (each * inverse for each in comp)
    dy1, dy2, dy3, dy4, dy5, dy6, dy7, dy8 = (dharm[m : m + 1, :] for m in range(8))
    grad_ux = ROOT_THREE * dy1 + ROOT_FIFTEEN * (uy * dy4 + uz * dy7 + ux * dy8) - ROOT_FIVE * ux * dy6
    grad_uy = ROOT_THREE * dy2 + ROOT_FIFTEEN * (ux * dy4 + uz * dy5 - uy * dy8) - ROOT_FIVE * uy * dy6
    grad_uz = ROOT_THREE * dy3 + ROOT_FIFTEEN * (uy * dy5 + ux * dy7) + 2.0 * ROOT_FIVE * uz * dy6
    along = ux * grad_ux + uy * grad_uy + uz * grad_uz
    grad_displace = jnp.concatenate(
        [
            (grad - unit * along) * inverse + grad_radius * unit
            for grad, unit in ((grad_ux, ux), (grad_uy, uy), (grad_uz, uz))
        ],
        0,
    )
    moved = grad_displace[:, 0:ATOMS]
    for slot in range(1, SLOTS):
        moved = moved + grad_displace[:, ATOMS * slot : ATOMS * slot + ATOMS]
    pieces = parts(grad_displace)
    where = blocks[0:1, :]
    for slot in range(BLOCKS):
        masked[16 * slot : 16 * slot + 16, :] = jnp.where(where == slot, pieces, 0.0).astype(BF16)
    drawn = dot(masked[...], inner[...], NT)
    own_place = joined(jnp.concatenate([drawn[0:16], drawn[16:32]], 1))
    blank = jnp.zeros((8, SEND), F32)
    pgrad[0, 4] = jnp.zeros((8, ATOMS), F32)
    for dx in (-1, 0, 1):
        for dy in (-1, 0, 1):
            for dz in (-1, 0, 1):
                if (dx, dy, dz) != (0, 0, 0):
                    slot = slot_of(dx, dy, dz)
                    pgrad[0 if dz == 0 else 1 + (dz > 0), column(dx, dy)] = jnp.concatenate(
                        [joined(drawn[16 * slot : 16 * slot + 16]), blank], 1
                    )
    for side in (-1, 1):
        start(back_place(2, side))

    for rank in (4, 0):
        keep_flats(rank)
    send_pairs(PAIR0, ORDER[0:2])

    def arrived_z(dx, dy):
        total = None
        for dz in (-1, 1):
            back_z(dx, dy, dz).wait_recv()
            which = slot_of(dx, dy, dz) - (2 if (dx, dy) == (0, 0) else PAIR0 // SEND - 2)
            value = zrecv[which].astype(F32)
            total = value if total is None else total + value
        if (dx, dy) == (0, 0):
            return total
        return total + flat_g[ORDER.index((dx, dy))]

    for dx, dy in (ORDER[4:] + ORDER[2:4]):
        xsend[3 * (dx > 0) + dy + 1] = arrived_z(dx, dy).astype(BF16)
        start(back_x(dx, dy))
    for side in (-1, 1):
        back_place(2, side).wait_recv()
    for side in (-1, 1):
        lines = pl.ds(3 + 3 * side, 3)
        pxsend[1 * (side > 0)] = pgrad[0, lines] + pzrecv[0, lines] + pzrecv[1, lines]
        start(back_place(0, side))

    rows = dot(drows[...], onehot[0:FLAT0, :], NT)
    own_g[...] = rows[:, 0:ATOMS] + dot(dlow[...], onehot[0:ATOMS, :], NT)
    for dz, value in zip((-1, 1), folded(rows[:, ATOMS:FLAT0])):
        zsend[1 * (dz > 0)] = value.astype(BF16)
        start(back_z(0, 0, dz))

    for dy in (-1, 1, 0):
        total = arrived_z(0, dy)
        for dx in (-1, 1):
            back_x(dx, dy).wait_recv()
            total = total + xrecv[3 * (dx > 0) + dy + 1].astype(F32)
        if dy:
            ysend[1 * (dy > 0)] = total.astype(BF16)
            start(back_y(dy))
        if dy == 1:
            for side in (-1, 1):
                back_place(0, side).wait_recv()
            middle = pl.ds(3, 3)
            totals = pgrad[0, middle]
            totals = totals + pzrecv[0, middle] + pzrecv[1, middle] + pxrecv[0] + pxrecv[1]
            pysend[0] = totals[0]
            pysend[1] = totals[2]
            for side in (-1, 1):
                start(back_place(1, side))
    for dy in (-1, 1):
        back_y(dy).wait_recv()
        total = total + yrecv[1 * (dy > 0)].astype(F32)
    high, rest = split(total)
    for part, chosen in enumerate((picks_left, picks_right)):
        rows = slice(HALF * part, HALF * part + HALF)
        own_g[rows, :] += dot(high, chosen, NT) + dot(rest, chosen, NT)
    for tile in range(4):
        rows = slice(128 * tile, 128 * tile + 128)
        high, rest = split(own_g[rows, :])
        fgrad_ref[rows, :] = dot(mix[tile], high) + dot(mix[tile], rest)
    high, rest = split(own_g[512:FEAT, :])
    fgrad_ref[512:FEAT, :] = dot(mix_ref[2], high) + dot(mix_ref[2], rest)

    back = totals[1]
    for side in (-1, 1):
        back_place(1, side).wait_recv()
        back = back + pyrecv[1 * (side > 0)]
    force = moved - own_place[0:3] - joined(dot(parts(back).astype(BF16), picks_left, NT))[0:3]
    for axis in range(3):
        force_ref[axis] = force[axis : axis + 1]
    for copy in started:
        copy.wait_send()


def shards(
    positions, features, species, neighbours, send_list, mix_weight, radial_in, radial_out, readout
):
    vmem = pl.BlockSpec(memory_space=pltpu.VMEM)
    energy, forces, feature_grad = pl.pallas_call(
        kernel,
        out_shape=(
            jax.ShapeDtypeStruct((1, ATOMS), F32),
            jax.ShapeDtypeStruct((3, 1, ATOMS), F32),
            jax.ShapeDtypeStruct((FEAT, ATOMS), F32),
        ),
        in_specs=[vmem] * 9,
        out_specs=(vmem, vmem, vmem),
        scratch_shapes=[
            pltpu.VMEM((HALF, 128), BF16),
            pltpu.VMEM((BLOCKS, HALF, 128), BF16),
            pltpu.VMEM((3, 9, 8, 128), F32),
            pltpu.VMEM((FEAT, ROWS), BF16),
            pltpu.VMEM((16 * BLOCKS, 128), BF16),
            pltpu.VMEM((ROWS, EDGES), BF16),
            pltpu.VMEM((SEND, EDGES), BF16),
            pltpu.VMEM((8, EDGES), jnp.int32),
            pltpu.VMEM((FEAT, EDGES), F32),
            pltpu.VMEM((FEAT, EDGES), BF16),
            pltpu.VMEM((8, EDGES), F32),
            pltpu.VMEM((8, EDGES), F32),
            pltpu.VMEM((SLOTS, ATOMS), jnp.int32),
            pltpu.VMEM((3 * CH, EDGES), F32),
            pltpu.VMEM((CH, EDGES), F32),
            pltpu.VMEM((8, EDGES), F32),
            pltpu.VMEM((8, EDGES), F32),
            pltpu.VMEM((FEAT, ATOMS), F32),
            pltpu.VMEM((FEAT, EDGES), BF16),
            pltpu.VMEM((FEAT, EDGES), BF16),
            pltpu.VMEM((3 * CH, EDGES), F32),
            pltpu.VMEM((8, EDGES), F32),
            pltpu.VMEM((16 * BLOCKS, EDGES), BF16),
            pltpu.VMEM((FEAT, ATOMS), F32),
            pltpu.VMEM((8, HALF, 128), F32),
            pltpu.VMEM((18, HALF, 128), BF16),
            pltpu.VMEM((18, HALF, 128), BF16),
            pltpu.VMEM((6, HALF, 128), BF16),
            pltpu.VMEM((6, HALF, 128), BF16),
            pltpu.VMEM((2, HALF, 128), BF16),
            pltpu.VMEM((2, HALF, 128), BF16),
            pltpu.VMEM((3, 9, 8, 128), F32),
            pltpu.VMEM((2, 9, 8, 128), F32),
            pltpu.VMEM((2, 3, 8, 128), F32),
            pltpu.VMEM((2, 3, 8, 128), F32),
            pltpu.VMEM((2, 8, 128), F32),
            pltpu.VMEM((2, 8, 128), F32),
            pltpu.SemaphoreType.DMA((BLOCKS,)),
            pltpu.SemaphoreType.DMA((BLOCKS,)),
            pltpu.SemaphoreType.DMA((BLOCKS,)),
            pltpu.SemaphoreType.DMA((BLOCKS,)),
            pltpu.SemaphoreType.DMA((12,)),
            pltpu.SemaphoreType.DMA((12,)),
        ],
        compiler_params=pltpu.CompilerParams(
            collective_id=0, has_side_effects=True, vmem_limit_bytes=60 * 1024 * 1024
        ),
        name="layer",
    )(
        positions.reshape(3, 1, ATOMS),
        features[0, 0, 0].T,
        species[0, 0],
        neighbours.reshape(SLOTS, 1, ATOMS),
        send_list[0, 0],
        mix_weight,
        radial_in,
        radial_out,
        jnp.transpose(readout, (1, 0, 2)),
    )
    return (
        energy[None, None],
        forces.reshape(1, 1, 1, 3, ATOMS),
        feature_grad.T[None, None, None],
    )


def solution(mesh):
    in_specs = (
        P("gx", "gy", "gz", None, None),
        P("gx", "gy", "gz", None, None),
        P("gx", "gy", "gz", None),
        P("gx", "gy", "gz", None, None),
        P("gx", "gy", "gz", None),
        P(),
        P(),
        P(),
        P(),
    )
    out_specs = (
        P("gx", "gy", "gz", None),
        P("gx", "gy", "gz", None, None),
        P("gx", "gy", "gz", None, None),
    )
    return jax.shard_map(shards, mesh=mesh, in_specs=in_specs, out_specs=out_specs, check_vma=False)
```

```python
import math

import jax
import jax.numpy as jnp
from jax import lax
from jax.experimental import pallas as pl
from jax.experimental.pallas import tpu as pltpu
from jax.sharding import PartitionSpec as P

EDGE = 3.0
HIGH = lax.Precision.HIGHEST
MESH = pl.DeviceIdType.MESH
LEVELS = (0, 1, 1, 1, 2, 2, 2, 2, 2)
ROOT_THREE = math.sqrt(3.0)
ROOT_FIVE = math.sqrt(5.0)
ROOT_FIFTEEN = math.sqrt(15.0)

ATOMS = 128
SEND = 64
SLOTS = 12
EDGES = SLOTS * ATOMS
CH = 64
FEAT = 576
HALF = 288
CHUNKS = 3
PIECE = HALF // CHUNKS
RUN = 4

ORDER = ((0, -1), (0, 1), (-1, 0), (1, 0), (-1, -1), (1, -1), (-1, 1), (1, 1))
FLAT0 = 256
PAIR0 = 768
ROWS = 1792
BLOCKS = ROWS // SEND

NN = (((1,), (0,)), ((), ()))
NT = (((1,), (1,)), ((), ()))
TN = (((0,), (0,)), ((), ()))
F32 = jnp.float32
BF16 = jnp.bfloat16


def dot(lhs, rhs, dims=NN, precision=None):
    return lax.dot_general(lhs, rhs, dims, precision=precision, preferred_element_type=F32)


def column(dx, dy):
    return (dx + 1) * 3 + dy + 1


def slot_of(dx, dy, dz):
    if (dx, dy) == (0, 0):
        return 2 + (dz > 0)
    rank = ORDER.index((dx, dy))
    if dz == 0:
        return FLAT0 // SEND + rank
    return PAIR0 // SEND + 2 * rank + (dz > 0)


def parts(value):
    first = value[0:3].astype(BF16).astype(F32)
    rest = value[0:3] - first
    second = rest.astype(BF16).astype(F32)
    filler = jnp.zeros((7, value.shape[1]), F32)
    return jnp.concatenate([first, second, rest - second, filler], 0)


def joined(rows):
    total = rows[0:3] + rows[3:6] + rows[6:9]
    return jnp.concatenate([total, jnp.zeros((5, rows.shape[1]), F32)], 0)


def split(value):
    high = value.astype(BF16)
    return high, (value - high.astype(F32)).astype(BF16)


def mixers(mix_ref):
    zero = jnp.zeros((CH, CH), BF16)

    def pair(upper, lower):
        return jnp.concatenate(
            [
                jnp.concatenate([mix_ref[upper], zero], 1),
                jnp.concatenate([zero, mix_ref[lower]], 1),
            ],
            0,
        )

    last = pair(2, 2)
    return (pair(0, 1), pair(1, 1), last, last)


def kernel(
    *refs,
):
    arguments, refs = refs[:9], refs[9:]
    (
        energy_ref,
        force_ref,
        owned_ref,
        pos_ref,
        feat_ref,
        spec_ref,
        nbr_ref,
        list_ref,
        mix_ref,
        rin_ref,
        rout_ref,
        read_ref,
        shared,
        ghosts,
        place,
        tbl,
        prows,
        onehot,
        inner,
        blocks,
        total_g,
        gath,
        placed,
        base,
        index,
        radial,
        pre,
        harm,
        basis_ref,
        accum,
        drows,
        dlow,
        drad,
        dharm,
        masked,
        own_g,
        flat_g,
        zsend,
        zrecv,
        xsend,
        xrecv,
        ysend,
        yrecv,
        pgrad,
        pzrecv,
        pxsend,
        pxrecv,
        pysend,
        pyrecv,
        fsend_sem,
        frecv_sem,
        bsend_sem,
        brecv_sem,
        psend_sem,
        precv_sem,
        load_sem,
    ) = refs
    size_x, size_y, size_z = (lax.axis_size(name) for name in ("gx", "gy", "gz"))
    me_x, me_y, me_z = (lax.axis_index(name) for name in ("gx", "gy", "gz"))
    run_at = lax.rem(me_x, RUN)
    bend = {-1: -jnp.where(run_at == 0, 1, 0), 1: jnp.where(run_at == RUN - 1, 1, 0)}

    def device(dx, dy, dz):
        turn = bend[dx] if dx else 0
        return (
            lax.rem(me_x + dx + size_x, size_x),
            lax.rem(me_y + dy + turn + size_y, size_y),
            lax.rem(me_z + dz + size_z, size_z),
        )

    sides = ((0, -1, 0), (0, 1, 0), (-1, 0, 0), (1, 0, 0), (0, 0, -1), (0, 0, 1))
    barrier = pltpu.get_barrier_semaphore()
    for side in sides:
        pl.semaphore_signal(barrier, inc=1, device_id=device(*side), device_id_type=MESH)

    inputs = (pos_ref, feat_ref, spec_ref, nbr_ref, list_ref, mix_ref, rin_ref, rout_ref, read_ref)
    loads = [
        pltpu.make_async_copy(source, target, load_sem.at[which])
        for which, (source, target) in enumerate(zip(arguments, inputs))
    ]
    for load in loads:
        load.start()
    for load in loads:
        load.wait()

    mix = mixers(mix_ref)
    pos8 = jnp.concatenate([pos_ref[0], pos_ref[1], pos_ref[2], jnp.zeros((5, ATOMS), F32)], 0)
    for tile in range(4):
        rows = slice(128 * tile, 128 * tile + 128)
        tbl[rows, 0:ATOMS] = dot(mix[tile], feat_ref[rows, :], TN).astype(BF16)
    tbl[512:FEAT, 0:ATOMS] = dot(mix_ref[2], feat_ref[512:FEAT, :], TN).astype(BF16)
    picks = jnp.where(
        lax.broadcasted_iota(jnp.int32, (ATOMS, SEND), 0) == list_ref[...], 1.0, 0.0
    ).astype(BF16)
    zero = jnp.zeros((ATOMS, SEND), BF16)
    picks_left = jnp.concatenate([picks, zero], 1)
    picks_right = jnp.concatenate([zero, picks], 1)
    shared[...] = (
        dot(tbl[0:HALF, 0:ATOMS], picks_left) + dot(tbl[HALF:FEAT, 0:ATOMS], picks_right)
    ).astype(BF16)
    pos_parts = parts(pos8).astype(BF16)
    place[0, 4] = joined(dot(pos_parts, picks_left))

    pl.semaphore_wait(barrier, len(sides))

    started = []

    def start(copy):
        copy.start()
        started.append(copy)

    def remote(source, target, sends, recvs, which, go):
        return pltpu.make_async_remote_copy(
            src_ref=source,
            dst_ref=target,
            send_sem=sends.at[which],
            recv_sem=recvs.at[which],
            device_id=device(*go),
            device_id_type=MESH,
        )

    def piece(chunk):
        return pl.ds(PIECE * chunk, PIECE)

    def halo(dx, dy, dz, axis, chunk):
        go = [0, 0, 0]
        go[axis] = -(dx, dy, dz)[axis]
        origin = [dx, dy, dz]
        origin[axis] = 0
        part = piece(chunk)
        source = ghosts.at[slot_of(*origin), part] if any(origin) else shared.at[part]
        slot = slot_of(dx, dy, dz)
        target = ghosts.at[slot, part]
        return remote(source, target, fsend_sem, frecv_sem, CHUNKS * slot + chunk, go)

    def wait_halo(dx, dy, dz, axis):
        for chunk in range(CHUNKS):
            halo(dx, dy, dz, axis, chunk).wait_recv()

    def halo_place(axis, side):
        which = 2 * axis + (side > 0)
        if axis == 1:
            source, target, go = place.at[0, 4], place.at[0, 4 + side], (0, -side, 0)
        elif axis == 0:
            source, target = place.at[0, pl.ds(3, 3)], place.at[0, pl.ds(3 + 3 * side, 3)]
            go = (-side, 0, 0)
        else:
            source, target, go = place.at[0], place.at[1 + (side > 0)], (0, 0, -side)
        return remote(source, target, psend_sem, precv_sem, which, go)

    for side in (-1, 1):
        start(halo_place(1, side))
    for chunk in range(CHUNKS):
        for dy in (-1, 1):
            start(halo(0, dy, 0, 1, chunk))
    for chunk in range(CHUNKS):
        for dx in (-1, 1):
            start(halo(dx, 0, 0, 0, chunk))
    for chunk in range(CHUNKS):
        for dz in (-1, 1):
            start(halo(0, 0, dz, 2, chunk))

    near = jnp.concatenate([nbr_ref[slot] for slot in range(SLOTS)], 0)
    ghost = near - ATOMS
    block = ghost >> 6
    step_x = (block * 57) >> 9
    line = (block * 43) >> 7
    step_y = line - 3 * step_x
    step_z = block - 3 * line
    through = step_y - jnp.where(step_x == 0, bend[-1], jnp.where(step_x == 2, bend[1], 0))
    through = jnp.where(through < 0, through + 3, jnp.where(through > 2, through - 3, through))
    spot = 3 * step_x + through
    flat = jnp.zeros_like(spot)
    paired = jnp.full_like(spot, ATOMS)
    for rank, (dx, dy) in enumerate(ORDER):
        here = spot == column(dx, dy)
        flat = jnp.where(here, FLAT0 + SEND * rank, flat)
        paired = jnp.where(here, PAIR0 + 2 * SEND * rank, paired)
    paired = paired + jnp.where(step_z > 1, SEND, 0)
    own = near < ATOMS
    row = jnp.where(own, near, jnp.where(step_z == 1, flat, paired) + (ghost & 63))
    index[...] = row
    shifts = [
        jnp.where(own, 0.0, EDGE * (step - 1).astype(F32)) for step in (step_x, step_y, step_z)
    ]
    for slot in range(SLOTS):
        lanes = slice(128 * slot, 128 * slot + 128)
        blocks[0:1, lanes] = row[slot : slot + 1] >> 6
        base[:, lanes] = (
            jnp.concatenate([each[slot : slot + 1] for each in shifts] + [jnp.zeros((5, ATOMS), F32)], 0)
            - pos8
        )

    rows_iota = lax.broadcasted_iota(jnp.int32, (ATOMS, ATOMS), 0)

    def fill(slot, carry):
        lanes = pl.ds(pl.multiple_of(slot * ATOMS, ATOMS), ATOMS)
        wanted = index[pl.ds(slot, 1), :]
        inner[:, lanes] = jnp.where(rows_iota[0:SEND] == (wanted & 63), 1.0, 0.0).astype(BF16)
        for part in range(ROWS // ATOMS):
            onehot[part * ATOMS : (part + 1) * ATOMS, lanes] = jnp.where(
                rows_iota == wanted - part * ATOMS, 1.0, 0.0
            ).astype(BF16)
        return carry

    lax.fori_loop(0, SLOTS, fill, 0)

    def settle(row, left, right):
        lanes = slice(row, row + 128)
        for part in range(2):
            half = slice(SEND * part, SEND * part + SEND)
            tbl[HALF * part : HALF * part + HALF, lanes] = jnp.concatenate(
                [ghosts[left][:, half], ghosts[right][:, half]], 1
            )

    def settle_pair(dx, dy):
        left, right = slot_of(dx, dy, -1), slot_of(dx, dy, 1)
        settle(SEND * left, left, right)

    def gather(low, high):
        def one(step, carry):
            lanes = pl.ds(pl.multiple_of(step * 256, 256), 256)
            rows = dot(tbl[:, low:high], onehot[low:high, lanes])
            if low:
                rows = rows + total_g[:, lanes]
            if high == ROWS:
                gath[:, lanes] = rows.astype(BF16)
            else:
                total_g[:, lanes] = rows
            return carry

        lax.fori_loop(0, EDGES // 256, one, 0)

    for side in (-1, 1):
        halo_place(1, side).wait_recv()
    for side in (-1, 1):
        start(halo_place(0, side))
    def pass_x(dy, chunk):
        halo(0, dy, 0, 1, chunk).wait_recv()
        for dx in (-1, 1):
            start(halo(dx, dy, 0, 0, chunk))
        for dz in (-1, 1):
            start(halo(0, dy, dz, 2, chunk))

    def pass_z(dx, dy, chunk):
        halo(dx, dy, 0, 0, chunk).wait_recv()
        for dz in (-1, 1):
            start(halo(dx, dy, dz, 2, chunk))

    for chunk in range(CHUNKS):
        for dy in (-1, 1):
            pass_x(dy, chunk)
    for side in (-1, 1):
        halo_place(0, side).wait_recv()
    for side in (-1, 1):
        start(halo_place(2, side))
    for chunk in range(CHUNKS):
        for dx in (-1, 1):
            pass_z(dx, 0, chunk)
    for dz in (-1, 1):
        wait_halo(0, 0, dz, 2)
    settle_pair(0, 0)
    gather(0, FLAT0)
    for chunk in range(CHUNKS):
        for dy in (-1, 1):
            for dx in (-1, 1):
                pass_z(dx, dy, chunk)
    for rank in range(0, 8, 2):
        left = FLAT0 // SEND + rank
        settle(SEND * left, left, left + 1)
    gather(FLAT0, PAIR0)

    for side in (-1, 1):
        halo_place(2, side).wait_recv()
    for half in range(2):
        prows[16 * half : 16 * half + 16, 0:SEND] = pos_parts[:, SEND * half : SEND * half + SEND]
    for dx in (-1, 0, 1):
        for dy in (-1, 0, 1):
            for dz in (-1, 0, 1):
                if (dx, dy, dz) != (0, 0, 0):
                    slot = slot_of(dx, dy, dz)
                    prows[16 * slot : 16 * slot + 16, :] = parts(
                        place[0 if dz == 0 else 1 + (dz > 0), column(dx, dy)]
                    ).astype(BF16)

    def locate(step, carry):
        lanes = pl.ds(pl.multiple_of(step * 256, 256), 256)
        rows = dot(prows[:, 0:SEND], inner[:, lanes])
        where = blocks[0:1, lanes]
        chosen = jnp.zeros((16, 256), F32)
        for slot in range(BLOCKS):
            chosen = jnp.where(where == slot, rows[16 * slot : 16 * slot + 16], chosen)
        placed[:, lanes] = joined(chosen)
        return carry

    lax.fori_loop(0, EDGES // 256, locate, 0)
    displace = placed[...] + base[...]
    comp = [displace[axis : axis + 1] for axis in range(3)]
    radius = jnp.sqrt(comp[0] * comp[0] + comp[1] * comp[1] + comp[2] * comp[2] + 1.0)
    inverse = 1.0 / radius
    ux, uy, uz = (each * inverse for each in comp)
    harm[0:8, :] = jnp.concatenate(
        [
            ROOT_THREE * ux,
            ROOT_THREE * uy,
            ROOT_THREE * uz,
            ROOT_FIFTEEN * ux * uy,
            ROOT_FIFTEEN * uy * uz,
            0.5 * ROOT_FIVE * (2.0 * uz * uz - ux * ux - uy * uy),
            ROOT_FIFTEEN * ux * uz,
            0.5 * ROOT_FIFTEEN * (ux * ux - uy * uy),
        ],
        0,
    )
    spacing = radius - 1.25 * lax.broadcasted_iota(jnp.int32, (8, EDGES), 0).astype(F32)
    basis = jnp.exp(-0.5 * spacing * spacing)
    basis_ref[...] = basis * spacing
    before = dot(rin_ref[...], basis, TN, HIGH)
    pre[...] = before
    hidden = before / (1.0 + jnp.exp(-before))
    radial[...] = dot(rout_ref[...], hidden, TN, HIGH)

    for dx, dy in ORDER[:4]:
        for dz in (-1, 1):
            wait_halo(dx, dy, dz, 2)
        settle_pair(dx, dy)
    gather(PAIR0, PAIR0 + 512)
    for dx, dy in ORDER[4:]:
        for dz in (-1, 1):
            wait_halo(dx, dy, dz, 2)
        settle_pair(dx, dy)
    gather(PAIR0 + 512, ROWS)

    accum[...] = jnp.zeros((FEAT, ATOMS), F32)

    def forward(slot, carry):
        lanes = pl.ds(pl.multiple_of(slot * ATOMS, ATOMS), ATOMS)
        for part in range(4):
            low = 16 * part
            first = gath[low : low + 16, lanes].astype(F32)
            for m in range(9):
                rows = slice(CH * m + low, CH * m + low + 16)
                weight = radial[CH * LEVELS[m] + low : CH * LEVELS[m] + low + 16, lanes]
                if m == 0:
                    value = first + first
                else:
                    value = harm[m - 1 : m, lanes] * first + gath[rows, lanes].astype(F32)
                accum[rows, :] += weight * value
        return carry

    lax.fori_loop(0, SLOTS, forward, 0)

    norm = 1.0 / math.sqrt(SLOTS)
    kinds = (spec_ref[...] == 1).astype(F32)
    by_kind = jnp.concatenate([1.0 - kinds, kinds], 0)
    energy = jnp.zeros((1, ATOMS), F32)
    for level in range(3):
        weight = dot(read_ref[level], by_kind, TN, HIGH)
        total = jnp.zeros((CH, ATOMS), F32)
        for m in range(9):
            if LEVELS[m] != level:
                continue
            rows = slice(CH * m, CH * m + CH)
            value = accum[rows, :] * norm
            if level == 0:
                total = value
                accum[rows, :] = weight * norm
            else:
                total = total + value * value
                accum[rows, :] = (2.0 * norm) * weight * value
        energy = energy + jnp.sum(weight * total, 0, keepdims=True)
    energy_ref[...] = energy

    def backward(slot, carry):
        lanes = pl.ds(pl.multiple_of(slot * ATOMS, ATOMS), ATOMS)
        turns = [None] * 9
        for part in range(4):
            low = 16 * part
            first = gath[low : low + 16, lanes].astype(F32)
            weights = [radial[CH * l + low : CH * l + low + 16, lanes] for l in range(3)]
            slope = accum[low : low + 16, :]
            grad_first = 2.0 * (slope * weights[0])
            grad_radial = [2.0 * (slope * first), None, None]
            for m in range(1, 9):
                level = LEVELS[m]
                rows = slice(CH * m + low, CH * m + low + 16)
                slope = accum[rows, :]
                turn = harm[m - 1 : m, lanes]
                weighted = slope * weights[level]
                high, rest = split(weighted)
                drows[rows, lanes] = high
                dlow[rows, lanes] = rest
                grad_first = grad_first + weighted * turn
                term = slope * (turn * first + gath[rows, lanes].astype(F32))
                grad_radial[level] = term if grad_radial[level] is None else grad_radial[level] + term
                spin = weighted * first
                turns[m] = spin if turns[m] is None else turns[m] + spin
            high, rest = split(grad_first)
            drows[low : low + 16, lanes] = high
            dlow[low : low + 16, lanes] = rest
            for level in range(3):
                drad[CH * level + low : CH * level + low + 16, lanes] = grad_radial[level]
        dharm[:, lanes] = jnp.concatenate(
            [jnp.sum(turns[m], 0, keepdims=True) for m in range(1, 9)], 0
        )
        return carry

    lax.fori_loop(0, SLOTS, backward, 0)

    def lane_z(dx, dy, dz):
        return slot_of(dx, dy, dz) - (2 if (dx, dy) == (0, 0) else PAIR0 // SEND - 2)

    def lane_x(dx, dy):
        return 3 * (dx > 0) + dy + 1

    def back(sends, recvs, lane, slot, chunk, go):
        part = piece(chunk)
        return remote(
            sends.at[lane, part],
            recvs.at[lane, part],
            bsend_sem,
            brecv_sem,
            CHUNKS * slot + chunk,
            go,
        )

    def back_z(dx, dy, dz, chunk):
        lane = lane_z(dx, dy, dz)
        return back(zsend, zrecv, lane, slot_of(dx, dy, dz), chunk, (0, 0, dz))

    def back_x(dx, dy, chunk):
        return back(xsend, xrecv, lane_x(dx, dy), slot_of(dx, dy, 0), chunk, (dx, 0, 0))

    def back_y(dy, chunk):
        return back(ysend, yrecv, 1 * (dy > 0), slot_of(0, dy, 0), chunk, (0, dy, 0))

    def back_place(axis, side):
        at = 1 * (side > 0)
        if axis == 2:
            source, target, go = pgrad.at[1 + at], pzrecv.at[at], (0, 0, side)
        elif axis == 0:
            source, target, go = pxsend.at[at], pxrecv.at[at], (side, 0, 0)
        else:
            source, target, go = pysend.at[at], pyrecv.at[at], (0, side, 0)
        return remote(source, target, psend_sem, precv_sem, 6 + 2 * axis + at, go)

    def folded(pair):
        return [
            jnp.concatenate(
                [pair[0:HALF, SEND * part : SEND * part + SEND], pair[HALF:FEAT, SEND * part : SEND * part + SEND]],
                1,
            )
            for part in range(2)
        ]

    def send_pairs(rank):
        row = PAIR0 + 128 * rank
        rows = dot(drows[...], onehot[row : row + 256, :], NT)
        for at in range(2):
            for dz, value in zip((-1, 1), folded(rows[:, 128 * at : 128 * at + 128])):
                zsend[lane_z(*ORDER[rank + at], dz)] = value.astype(BF16)
        for chunk in range(CHUNKS):
            for dx, dy in ORDER[rank : rank + 2]:
                for dz in (-1, 1):
                    start(back_z(dx, dy, dz, chunk))

    def keep_flats(rank):
        rows = dot(drows[...], onehot[FLAT0 + SEND * rank : FLAT0 + SEND * rank + 256, :], NT)
        for at in range(2):
            for part, value in enumerate(folded(rows[:, 128 * at : 128 * at + 128])):
                flat_g[rank + 2 * at + part] = value

    def arrived_z(dx, dy, chunk):
        rows = slice(PIECE * chunk, PIECE * chunk + PIECE)
        total = None
        for dz in (-1, 1):
            back_z(dx, dy, dz, chunk).wait_recv()
            value = zrecv[lane_z(dx, dy, dz), rows, :].astype(F32)
            total = value if total is None else total + value
        if (dx, dy) == (0, 0):
            return total
        return total + flat_g[ORDER.index((dx, dy)), rows, :]

    def arrived_x(dy, chunk):
        rows = slice(PIECE * chunk, PIECE * chunk + PIECE)
        total = arrived_z(0, dy, chunk)
        for dx in (-1, 1):
            back_x(dx, dy, chunk).wait_recv()
            total = total + xrecv[lane_x(dx, dy), rows, :].astype(F32)
        return total

    def send_x(rank):
        for chunk in range(CHUNKS):
            rows = slice(PIECE * chunk, PIECE * chunk + PIECE)
            for dx, dy in ORDER[rank : rank + 2]:
                xsend[lane_x(dx, dy), rows, :] = arrived_z(dx, dy, chunk).astype(BF16)
                start(back_x(dx, dy, chunk))

    def send_y(chunk):
        rows = slice(PIECE * chunk, PIECE * chunk + PIECE)
        for dy in (-1, 1):
            ysend[1 * (dy > 0), rows, :] = arrived_x(dy, chunk).astype(BF16)
            start(back_y(dy, chunk))

    send_pairs(4)
    send_pairs(6)
    keep_flats(4)
    send_pairs(0)
    keep_flats(0)
    send_pairs(2)
    send_x(4)
    send_x(6)

    before = pre[...]
    sigmoid = 1.0 / (1.0 + jnp.exp(-before))
    grad_hidden = dot(rout_ref[...], drad[...], NN, HIGH)
    grad_before = grad_hidden * (sigmoid * (1.0 + before * (1.0 - sigmoid)))
    grad_basis = dot(rin_ref[...], grad_before, NN, HIGH)
    grad_radius = jnp.sum(-(grad_basis * basis_ref[...]), 0, keepdims=True)
    displace = placed[...] + base[...]
    comp = [displace[axis : axis + 1] for axis in range(3)]
    radius = jnp.sqrt(comp[0] * comp[0] + comp[1] * comp[1] + comp[2] * comp[2] + 1.0)
    inverse = 1.0 / radius
    ux, uy, uz = (each * inverse for each in comp)
    dy1, dy2, dy3, dy4, dy5, dy6, dy7, dy8 = (dharm[m : m + 1, :] for m in range(8))
    grad_ux = ROOT_THREE * dy1 + ROOT_FIFTEEN * (uy * dy4 + uz * dy7 + ux * dy8) - ROOT_FIVE * ux * dy6
    grad_uy = ROOT_THREE * dy2 + ROOT_FIFTEEN * (ux * dy4 + uz * dy5 - uy * dy8) - ROOT_FIVE * uy * dy6
    grad_uz = ROOT_THREE * dy3 + ROOT_FIFTEEN * (uy * dy5 + ux * dy7) + 2.0 * ROOT_FIVE * uz * dy6
    along = ux * grad_ux + uy * grad_uy + uz * grad_uz
    grad_displace = jnp.concatenate(
        [
            (grad - unit * along) * inverse + grad_radius * unit
            for grad, unit in ((grad_ux, ux), (grad_uy, uy), (grad_uz, uz))
        ],
        0,
    )
    moved = grad_displace[:, 0:ATOMS]
    for slot in range(1, SLOTS):
        moved = moved + grad_displace[:, ATOMS * slot : ATOMS * slot + ATOMS]
    pieces = parts(grad_displace)
    where = blocks[0:1, :]
    for slot in range(BLOCKS):
        masked[16 * slot : 16 * slot + 16, :] = jnp.where(where == slot, pieces, 0.0).astype(BF16)
    drawn = dot(masked[...], inner[...], NT)
    own_place = joined(jnp.concatenate([drawn[0:16], drawn[16:32]], 1))
    blank = jnp.zeros((8, SEND), F32)
    pgrad[0, 4] = jnp.zeros((8, ATOMS), F32)
    for dx in (-1, 0, 1):
        for dy in (-1, 0, 1):
            for dz in (-1, 0, 1):
                if (dx, dy, dz) != (0, 0, 0):
                    slot = slot_of(dx, dy, dz)
                    pgrad[0 if dz == 0 else 1 + (dz > 0), column(dx, dy)] = jnp.concatenate(
                        [joined(drawn[16 * slot : 16 * slot + 16]), blank], 1
                    )
    for side in (-1, 1):
        start(back_place(2, side))

    send_x(2)
    rows = dot(drows[...], onehot[0:FLAT0, :], NT)
    own_g[...] = rows[:, 0:ATOMS] + dot(dlow[...], onehot[0:ATOMS, :], NT)
    for dz, value in zip((-1, 1), folded(rows[:, ATOMS:FLAT0])):
        zsend[lane_z(0, 0, dz)] = value.astype(BF16)
        for chunk in range(CHUNKS):
            start(back_z(0, 0, dz, chunk))

    for chunk in range(CHUNKS - 1):
        send_y(chunk)
    for side in (-1, 1):
        back_place(2, side).wait_recv()
    for side in (-1, 1):
        lines = pl.ds(3 + 3 * side, 3)
        pxsend[1 * (side > 0)] = pgrad[0, lines] + pzrecv[0, lines] + pzrecv[1, lines]
        start(back_place(0, side))
    send_y(CHUNKS - 1)
    for side in (-1, 1):
        back_place(0, side).wait_recv()
    middle = pl.ds(3, 3)
    totals = pgrad[0, middle] + pzrecv[0, middle] + pzrecv[1, middle] + pxrecv[0] + pxrecv[1]
    pysend[0] = totals[0]
    pysend[1] = totals[2]
    for side in (-1, 1):
        start(back_place(1, side))
    for chunk in range(CHUNKS):
        total = arrived_x(0, chunk)
        for dy in (-1, 1):
            back_y(dy, chunk).wait_recv()
            total = total + yrecv[1 * (dy > 0), PIECE * chunk : PIECE * chunk + PIECE, :].astype(F32)
        high, rest = split(total)
        for part, chosen in enumerate((picks_left, picks_right)):
            at = HALF * part + PIECE * chunk
            owned_ref[at : at + PIECE, :] = (
                own_g[at : at + PIECE, :] + dot(high, chosen, NT) + dot(rest, chosen, NT)
            )

    final = totals[1]
    for side in (-1, 1):
        back_place(1, side).wait_recv()
        final = final + pyrecv[1 * (side > 0)]
    force = moved - own_place[0:3] - joined(dot(parts(final).astype(BF16), picks_left, NT))[0:3]
    for axis in range(3):
        force_ref[axis] = force[axis : axis + 1]
    for copy in started:
        copy.wait_send()


def finish(energy_in, force_in, owned_in, mix_ref, energy_ref, force_ref, fgrad_ref):
    energy_ref[...] = energy_in[...]
    force_ref[...] = force_in[...]
    mix = mixers(mix_ref)
    for tile in range(4):
        rows = slice(128 * tile, 128 * tile + 128)
        high, rest = split(owned_in[rows, :])
        fgrad_ref[rows, :] = dot(mix[tile], high) + dot(mix[tile], rest)
    high, rest = split(owned_in[512:FEAT, :])
    fgrad_ref[512:FEAT, :] = dot(mix_ref[2], high) + dot(mix_ref[2], rest)


def shards(
    positions, features, species, neighbours, send_list, mix_weight, radial_in, radial_out, readout
):
    vmem = pl.BlockSpec(memory_space=pltpu.VMEM)
    results = (
        jax.ShapeDtypeStruct((1, ATOMS), F32),
        jax.ShapeDtypeStruct((3, 1, ATOMS), F32),
        jax.ShapeDtypeStruct((FEAT, ATOMS), F32),
    )
    arguments = (
        positions.reshape(3, 1, ATOMS),
        features[0, 0, 0].T,
        species[0, 0],
        neighbours.reshape(SLOTS, 1, ATOMS),
        send_list[0, 0],
        mix_weight,
        radial_in,
        radial_out,
        jnp.transpose(readout, (1, 0, 2)),
    )
    energy, forces, owned = pl.pallas_call(
        kernel,
        out_shape=results,
        in_specs=[pl.BlockSpec(memory_space=pltpu.HBM)] * 9,
        out_specs=(vmem, vmem, vmem),
        scratch_shapes=[pltpu.VMEM(each.shape, each.dtype) for each in arguments]
        + [
            pltpu.VMEM((HALF, 128), BF16),
            pltpu.VMEM((BLOCKS, HALF, 128), BF16),
            pltpu.VMEM((3, 9, 8, 128), F32),
            pltpu.VMEM((FEAT, ROWS), BF16),
            pltpu.VMEM((16 * BLOCKS, 128), BF16),
            pltpu.VMEM((ROWS, EDGES), BF16),
            pltpu.VMEM((SEND, EDGES), BF16),
            pltpu.VMEM((8, EDGES), jnp.int32),
            pltpu.VMEM((FEAT, EDGES), F32),
            pltpu.VMEM((FEAT, EDGES), BF16),
            pltpu.VMEM((8, EDGES), F32),
            pltpu.VMEM((8, EDGES), F32),
            pltpu.VMEM((SLOTS, ATOMS), jnp.int32),
            pltpu.VMEM((3 * CH, EDGES), F32),
            pltpu.VMEM((CH, EDGES), F32),
            pltpu.VMEM((8, EDGES), F32),
            pltpu.VMEM((8, EDGES), F32),
            pltpu.VMEM((FEAT, ATOMS), F32),
            pltpu.VMEM((FEAT, EDGES), BF16),
            pltpu.VMEM((FEAT, EDGES), BF16),
            pltpu.VMEM((3 * CH, EDGES), F32),
            pltpu.VMEM((8, EDGES), F32),
            pltpu.VMEM((16 * BLOCKS, EDGES), BF16),
            pltpu.VMEM((FEAT, ATOMS), F32),
            pltpu.VMEM((8, HALF, 128), F32),
            pltpu.VMEM((18, HALF, 128), BF16),
            pltpu.VMEM((18, HALF, 128), BF16),
            pltpu.VMEM((6, HALF, 128), BF16),
            pltpu.VMEM((6, HALF, 128), BF16),
            pltpu.VMEM((2, HALF, 128), BF16),
            pltpu.VMEM((2, HALF, 128), BF16),
            pltpu.VMEM((3, 9, 8, 128), F32),
            pltpu.VMEM((2, 9, 8, 128), F32),
            pltpu.VMEM((2, 3, 8, 128), F32),
            pltpu.VMEM((2, 3, 8, 128), F32),
            pltpu.VMEM((2, 8, 128), F32),
            pltpu.VMEM((2, 8, 128), F32),
            pltpu.SemaphoreType.DMA((CHUNKS * BLOCKS,)),
            pltpu.SemaphoreType.DMA((CHUNKS * BLOCKS,)),
            pltpu.SemaphoreType.DMA((CHUNKS * BLOCKS,)),
            pltpu.SemaphoreType.DMA((CHUNKS * BLOCKS,)),
            pltpu.SemaphoreType.DMA((12,)),
            pltpu.SemaphoreType.DMA((12,)),
            pltpu.SemaphoreType.DMA((9,)),
        ],
        compiler_params=pltpu.CompilerParams(
            collective_id=0, has_side_effects=True, vmem_limit_bytes=40 * 1024 * 1024
        ),
        name="layer",
    )(*[pltpu.with_memory_space_constraint(each, pltpu.HBM) for each in arguments])
    energy, forces, feature_grad = pl.pallas_call(
        finish,
        out_shape=results,
        in_specs=[vmem] * 4,
        out_specs=(vmem, vmem, vmem),
        compiler_params=pltpu.CompilerParams(vmem_limit_bytes=4 * 1024 * 1024),
        name="finish",
    )(energy, forces, owned, mix_weight)
    return (
        energy[None, None],
        forces.reshape(1, 1, 1, 3, ATOMS),
        feature_grad.T[None, None, None],
    )


def solution(mesh):
    in_specs = (
        P("gx", "gy", "gz", None, None),
        P("gx", "gy", "gz", None, None),
        P("gx", "gy", "gz", None),
        P("gx", "gy", "gz", None, None),
        P("gx", "gy", "gz", None),
        P(),
        P(),
        P(),
        P(),
    )
    out_specs = (
        P("gx", "gy", "gz", None),
        P("gx", "gy", "gz", None, None),
        P("gx", "gy", "gz", None, None),
    )
    return jax.shard_map(shards, mesh=mesh, in_specs=in_specs, out_specs=out_specs, check_vma=False)
```

```python
import math

import jax
import jax.numpy as jnp
from jax import lax
from jax.experimental import pallas as pl
from jax.experimental.pallas import tpu as pltpu
from jax.sharding import PartitionSpec as P

EDGE = 3.0
HIGH = lax.Precision.HIGHEST
MESH = pl.DeviceIdType.MESH
LEVELS = (0, 1, 1, 1, 2, 2, 2, 2, 2)
ROOT_THREE = math.sqrt(3.0)
ROOT_FIVE = math.sqrt(5.0)
ROOT_FIFTEEN = math.sqrt(15.0)

ATOMS = 128
SEND = 64
SLOTS = 12
EDGES = SLOTS * ATOMS
CH = 64
FEAT = 576
HALF = 288
CHUNKS = 2
PIECE = HALF // CHUNKS
RUN = 4

ORDER = ((0, -1), (0, 1), (-1, 0), (1, 0), (-1, -1), (1, -1), (-1, 1), (1, 1))
FLAT0 = 256
PAIR0 = 768
ROWS = 1792
BLOCKS = ROWS // SEND

NN = (((1,), (0,)), ((), ()))
NT = (((1,), (1,)), ((), ()))
TN = (((0,), (0,)), ((), ()))
F32 = jnp.float32
BF16 = jnp.bfloat16


def dot(lhs, rhs, dims=NN, precision=None):
    return lax.dot_general(lhs, rhs, dims, precision=precision, preferred_element_type=F32)


def column(dx, dy):
    return (dx + 1) * 3 + dy + 1


def slot_of(dx, dy, dz):
    if (dx, dy) == (0, 0):
        return 2 + (dz > 0)
    rank = ORDER.index((dx, dy))
    if dz == 0:
        return FLAT0 // SEND + rank
    return PAIR0 // SEND + 2 * rank + (dz > 0)


def parts(value):
    first = value[0:3].astype(BF16).astype(F32)
    rest = value[0:3] - first
    second = rest.astype(BF16).astype(F32)
    filler = jnp.zeros((7, value.shape[1]), F32)
    return jnp.concatenate([first, second, rest - second, filler], 0)


def joined(rows):
    total = rows[0:3] + rows[3:6] + rows[6:9]
    return jnp.concatenate([total, jnp.zeros((5, rows.shape[1]), F32)], 0)


def split(value):
    high = value.astype(BF16)
    return high, (value - high.astype(F32)).astype(BF16)


def mixers(mix_ref):
    zero = jnp.zeros((CH, CH), BF16)

    def pair(upper, lower):
        return jnp.concatenate(
            [
                jnp.concatenate([mix_ref[upper], zero], 1),
                jnp.concatenate([zero, mix_ref[lower]], 1),
            ],
            0,
        )

    last = pair(2, 2)
    return (pair(0, 1), pair(1, 1), last, last)


def kernel(
    *refs,
):
    arguments, refs = refs[:9], refs[9:]
    (
        energy_ref,
        force_ref,
        owned_ref,
        pos_ref,
        feat_ref,
        spec_ref,
        nbr_ref,
        list_ref,
        mix_ref,
        rin_ref,
        rout_ref,
        read_ref,
        shared,
        ghosts,
        place,
        tbl,
        prows,
        onehot,
        inner,
        blocks,
        total_g,
        gath,
        placed,
        base,
        index,
        radial,
        pre,
        harm,
        basis_ref,
        accum,
        drows,
        dlow,
        drad,
        dharm,
        masked,
        own_g,
        flat_g,
        zsend,
        zrecv,
        xsend,
        xrecv,
        ysend,
        yrecv,
        pgrad,
        pzrecv,
        pxsend,
        pxrecv,
        pysend,
        pyrecv,
        fsend_sem,
        frecv_sem,
        bsend_sem,
        brecv_sem,
        psend_sem,
        precv_sem,
        load_sem,
    ) = refs
    size_x, size_y, size_z = (lax.axis_size(name) for name in ("gx", "gy", "gz"))
    me_x, me_y, me_z = (lax.axis_index(name) for name in ("gx", "gy", "gz"))
    run_at = lax.rem(me_x, RUN)
    bend = {-1: -jnp.where(run_at == 0, 1, 0), 1: jnp.where(run_at == RUN - 1, 1, 0)}

    def device(dx, dy, dz):
        turn = bend[dx] if dx else 0
        return (
            lax.rem(me_x + dx + size_x, size_x),
            lax.rem(me_y + dy + turn + size_y, size_y),
            lax.rem(me_z + dz + size_z, size_z),
        )

    sides = ((0, -1, 0), (0, 1, 0), (-1, 0, 0), (1, 0, 0), (0, 0, -1), (0, 0, 1))
    barrier = pltpu.get_barrier_semaphore()
    for side in sides:
        pl.semaphore_signal(barrier, inc=1, device_id=device(*side), device_id_type=MESH)

    inputs = (pos_ref, feat_ref, spec_ref, nbr_ref, list_ref, mix_ref, rin_ref, rout_ref, read_ref)
    loads = [
        pltpu.make_async_copy(source, target, load_sem.at[which])
        for which, (source, target) in enumerate(zip(arguments, inputs))
    ]
    for load in loads:
        load.start()
    for load in loads:
        load.wait()

    mix = mixers(mix_ref)
    pos8 = jnp.concatenate([pos_ref[0], pos_ref[1], pos_ref[2], jnp.zeros((5, ATOMS), F32)], 0)
    for tile in range(4):
        rows = slice(128 * tile, 128 * tile + 128)
        tbl[rows, 0:ATOMS] = dot(mix[tile], feat_ref[rows, :], TN).astype(BF16)
    tbl[512:FEAT, 0:ATOMS] = dot(mix_ref[2], feat_ref[512:FEAT, :], TN).astype(BF16)
    picks = jnp.where(
        lax.broadcasted_iota(jnp.int32, (ATOMS, SEND), 0) == list_ref[...], 1.0, 0.0
    ).astype(BF16)
    zero = jnp.zeros((ATOMS, SEND), BF16)
    picks_left = jnp.concatenate([picks, zero], 1)
    picks_right = jnp.concatenate([zero, picks], 1)
    shared[...] = (
        dot(tbl[0:HALF, 0:ATOMS], picks_left) + dot(tbl[HALF:FEAT, 0:ATOMS], picks_right)
    ).astype(BF16)
    pos_parts = parts(pos8).astype(BF16)
    place[0, 4] = joined(dot(pos_parts, picks_left))

    pl.semaphore_wait(barrier, len(sides))

    started = []

    def start(copy):
        copy.start()
        started.append(copy)

    def drain():
        for copy in started:
            copy.wait_send()
        started.clear()

    def remote(source, target, sends, recvs, which, go):
        return pltpu.make_async_remote_copy(
            src_ref=source,
            dst_ref=target,
            send_sem=sends.at[which],
            recv_sem=recvs.at[which],
            device_id=device(*go),
            device_id_type=MESH,
        )

    def piece(chunk):
        return pl.ds(PIECE * chunk, PIECE)

    def halo(dx, dy, dz, axis, chunk):
        go = [0, 0, 0]
        go[axis] = -(dx, dy, dz)[axis]
        origin = [dx, dy, dz]
        origin[axis] = 0
        part = piece(chunk)
        source = ghosts.at[slot_of(*origin), part] if any(origin) else shared.at[part]
        slot = slot_of(dx, dy, dz)
        target = ghosts.at[slot, part]
        return remote(source, target, fsend_sem, frecv_sem, CHUNKS * slot + chunk, go)

    def wait_halo(dx, dy, dz, axis):
        for chunk in range(CHUNKS):
            halo(dx, dy, dz, axis, chunk).wait_recv()

    def halo_place(axis, side):
        which = 2 * axis + (side > 0)
        if axis == 1:
            source, target, go = place.at[0, 4], place.at[0, 4 + side], (0, -side, 0)
        elif axis == 0:
            source, target = place.at[0, pl.ds(3, 3)], place.at[0, pl.ds(3 + 3 * side, 3)]
            go = (-side, 0, 0)
        else:
            source, target, go = place.at[0], place.at[1 + (side > 0)], (0, 0, -side)
        return remote(source, target, psend_sem, precv_sem, which, go)

    for side in (-1, 1):
        start(halo_place(1, side))
    for dy in (-1, 1):
        start(halo(0, dy, 0, 1, 0))
    for chunk in range(CHUNKS):
        for dz in (-1, 1):
            start(halo(0, 0, dz, 2, chunk))

    near = jnp.concatenate([nbr_ref[slot] for slot in range(SLOTS)], 0)
    ghost = near - ATOMS
    block = ghost >> 6
    step_x = (block * 57) >> 9
    line = (block * 43) >> 7
    step_y = line - 3 * step_x
    step_z = block - 3 * line
    through = step_y - jnp.where(step_x == 0, bend[-1], jnp.where(step_x == 2, bend[1], 0))
    through = jnp.where(through < 0, through + 3, jnp.where(through > 2, through - 3, through))
    spot = 3 * step_x + through
    flat = jnp.zeros_like(spot)
    paired = jnp.full_like(spot, ATOMS)
    for rank, (dx, dy) in enumerate(ORDER):
        here = spot == column(dx, dy)
        flat = jnp.where(here, FLAT0 + SEND * rank, flat)
        paired = jnp.where(here, PAIR0 + 2 * SEND * rank, paired)
    paired = paired + jnp.where(step_z > 1, SEND, 0)
    own = near < ATOMS
    row = jnp.where(own, near, jnp.where(step_z == 1, flat, paired) + (ghost & 63))
    index[...] = row
    shifts = [
        jnp.where(own, 0.0, EDGE * (step - 1).astype(F32)) for step in (step_x, step_y, step_z)
    ]
    for slot in range(SLOTS):
        lanes = slice(128 * slot, 128 * slot + 128)
        blocks[0:1, lanes] = row[slot : slot + 1] >> 6
        base[:, lanes] = (
            jnp.concatenate([each[slot : slot + 1] for each in shifts] + [jnp.zeros((5, ATOMS), F32)], 0)
            - pos8
        )

    rows_iota = lax.broadcasted_iota(jnp.int32, (ATOMS, ATOMS), 0)

    def fill(slot, carry):
        lanes = pl.ds(pl.multiple_of(slot * ATOMS, ATOMS), ATOMS)
        wanted = index[pl.ds(slot, 1), :]
        inner[:, lanes] = jnp.where(rows_iota[0:SEND] == (wanted & 63), 1.0, 0.0).astype(BF16)
        for part in range(ROWS // ATOMS):
            onehot[part * ATOMS : (part + 1) * ATOMS, lanes] = jnp.where(
                rows_iota == wanted - part * ATOMS, 1.0, 0.0
            ).astype(BF16)
        return carry

    lax.fori_loop(0, SLOTS, fill, 0)

    def settle(row, left, right):
        lanes = slice(row, row + 128)
        for part in range(2):
            half = slice(SEND * part, SEND * part + SEND)
            tbl[HALF * part : HALF * part + HALF, lanes] = jnp.concatenate(
                [ghosts[left][:, half], ghosts[right][:, half]], 1
            )

    def settle_pair(dx, dy):
        left, right = slot_of(dx, dy, -1), slot_of(dx, dy, 1)
        settle(SEND * left, left, right)

    def gather(low, high):
        def one(step, carry):
            lanes = pl.ds(pl.multiple_of(step * 256, 256), 256)
            rows = dot(tbl[:, low:high], onehot[low:high, lanes])
            if low:
                rows = rows + total_g[:, lanes]
            if high == ROWS:
                gath[:, lanes] = rows.astype(BF16)
            else:
                total_g[:, lanes] = rows
            return carry

        lax.fori_loop(0, EDGES // 256, one, 0)

    def pass_x(dy, chunk):
        halo(0, dy, 0, 1, chunk).wait_recv()
        for dx in (-1, 1):
            start(halo(dx, dy, 0, 0, chunk))
        for dz in (-1, 1):
            start(halo(0, dy, dz, 2, chunk))

    def pass_z(dx, dy, chunk):
        halo(dx, dy, 0, 0, chunk).wait_recv()
        for dz in (-1, 1):
            start(halo(dx, dy, dz, 2, chunk))

    drain()
    for chunk in range(1, CHUNKS):
        for dy in (-1, 1):
            start(halo(0, dy, 0, 1, chunk))
        for dz in (-1, 1):
            halo(0, 0, dz, 2, chunk - 1).wait_recv()
        if chunk == CHUNKS - 1:
            for dz in (-1, 1):
                halo(0, 0, dz, 2, chunk).wait_recv()
            settle_pair(0, 0)
            gather(0, FLAT0)
        drain()
    for side in (-1, 1):
        halo_place(1, side).wait_recv()
    for side in (-1, 1):
        start(halo_place(0, side))
    for chunk in range(CHUNKS):
        for dx in (-1, 1):
            start(halo(dx, 0, 0, 0, chunk))
    for dy in (-1, 1):
        pass_x(dy, 0)
    for side in (-1, 1):
        halo_place(0, side).wait_recv()
    for side in (-1, 1):
        start(halo_place(2, side))
    for chunk in range(1, CHUNKS):
        for dy in (-1, 1):
            pass_x(dy, chunk)
    for chunk in range(CHUNKS):
        for dx in (-1, 1):
            pass_z(dx, 0, chunk)
    for side in (-1, 1):
        halo_place(2, side).wait_recv()
    for half in range(2):
        prows[16 * half : 16 * half + 16, 0:SEND] = pos_parts[:, SEND * half : SEND * half + SEND]
    for dx in (-1, 0, 1):
        for dy in (-1, 0, 1):
            for dz in (-1, 0, 1):
                if (dx, dy, dz) != (0, 0, 0):
                    slot = slot_of(dx, dy, dz)
                    prows[16 * slot : 16 * slot + 16, :] = parts(
                        place[0 if dz == 0 else 1 + (dz > 0), column(dx, dy)]
                    ).astype(BF16)

    def locate(step, carry):
        lanes = pl.ds(pl.multiple_of(step * 256, 256), 256)
        rows = dot(prows[:, 0:SEND], inner[:, lanes])
        where = blocks[0:1, lanes]
        chosen = jnp.zeros((16, 256), F32)
        for slot in range(BLOCKS):
            chosen = jnp.where(where == slot, rows[16 * slot : 16 * slot + 16], chosen)
        placed[:, lanes] = joined(chosen)
        return carry

    lax.fori_loop(0, EDGES // 256, locate, 0)
    displace = placed[...] + base[...]
    comp = [displace[axis : axis + 1] for axis in range(3)]
    radius = jnp.sqrt(comp[0] * comp[0] + comp[1] * comp[1] + comp[2] * comp[2] + 1.0)
    inverse = 1.0 / radius
    ux, uy, uz = (each * inverse for each in comp)
    harm[0:8, :] = jnp.concatenate(
        [
            ROOT_THREE * ux,
            ROOT_THREE * uy,
            ROOT_THREE * uz,
            ROOT_FIFTEEN * ux * uy,
            ROOT_FIFTEEN * uy * uz,
            0.5 * ROOT_FIVE * (2.0 * uz * uz - ux * ux - uy * uy),
            ROOT_FIFTEEN * ux * uz,
            0.5 * ROOT_FIFTEEN * (ux * ux - uy * uy),
        ],
        0,
    )
    spacing = radius - 1.25 * lax.broadcasted_iota(jnp.int32, (8, EDGES), 0).astype(F32)
    basis = jnp.exp(-0.5 * spacing * spacing)
    basis_ref[...] = basis * spacing
    before = dot(rin_ref[...], basis, TN, HIGH)
    pre[...] = before
    hidden = before / (1.0 + jnp.exp(-before))
    radial[...] = dot(rout_ref[...], hidden, TN, HIGH)

    for chunk in range(CHUNKS):
        for dy in (-1, 1):
            for dx in (-1, 1):
                pass_z(dx, dy, chunk)
    for rank in range(0, 8, 2):
        left = FLAT0 // SEND + rank
        settle(SEND * left, left, left + 1)
    gather(FLAT0, PAIR0)

    for dx, dy in ORDER[:4]:
        for dz in (-1, 1):
            wait_halo(dx, dy, dz, 2)
        settle_pair(dx, dy)
    gather(PAIR0, PAIR0 + 512)
    for dx, dy in ORDER[4:]:
        for dz in (-1, 1):
            wait_halo(dx, dy, dz, 2)
        settle_pair(dx, dy)
    gather(PAIR0 + 512, ROWS)

    accum[...] = jnp.zeros((FEAT, ATOMS), F32)

    def forward(slot, carry):
        lanes = pl.ds(pl.multiple_of(slot * ATOMS, ATOMS), ATOMS)
        for part in range(4):
            low = 16 * part
            first = gath[low : low + 16, lanes].astype(F32)
            for m in range(9):
                rows = slice(CH * m + low, CH * m + low + 16)
                weight = radial[CH * LEVELS[m] + low : CH * LEVELS[m] + low + 16, lanes]
                if m == 0:
                    value = first + first
                else:
                    value = harm[m - 1 : m, lanes] * first + gath[rows, lanes].astype(F32)
                accum[rows, :] += weight * value
        return carry

    lax.fori_loop(0, SLOTS, forward, 0)

    norm = 1.0 / math.sqrt(SLOTS)
    kinds = (spec_ref[...] == 1).astype(F32)
    by_kind = jnp.concatenate([1.0 - kinds, kinds], 0)
    energy = jnp.zeros((1, ATOMS), F32)
    for level in range(3):
        weight = dot(read_ref[level], by_kind, TN, HIGH)
        total = jnp.zeros((CH, ATOMS), F32)
        for m in range(9):
            if LEVELS[m] != level:
                continue
            rows = slice(CH * m, CH * m + CH)
            value = accum[rows, :] * norm
            if level == 0:
                total = value
                accum[rows, :] = weight * norm
            else:
                total = total + value * value
                accum[rows, :] = (2.0 * norm) * weight * value
        energy = energy + jnp.sum(weight * total, 0, keepdims=True)
    energy_ref[...] = energy

    def backward(slot, carry):
        lanes = pl.ds(pl.multiple_of(slot * ATOMS, ATOMS), ATOMS)
        turns = [None] * 9
        for part in range(4):
            low = 16 * part
            first = gath[low : low + 16, lanes].astype(F32)
            weights = [radial[CH * l + low : CH * l + low + 16, lanes] for l in range(3)]
            slope = accum[low : low + 16, :]
            grad_first = 2.0 * (slope * weights[0])
            grad_radial = [2.0 * (slope * first), None, None]
            for m in range(1, 9):
                level = LEVELS[m]
                rows = slice(CH * m + low, CH * m + low + 16)
                slope = accum[rows, :]
                turn = harm[m - 1 : m, lanes]
                weighted = slope * weights[level]
                high, rest = split(weighted)
                drows[rows, lanes] = high
                dlow[rows, lanes] = rest
                grad_first = grad_first + weighted * turn
                term = slope * (turn * first + gath[rows, lanes].astype(F32))
                grad_radial[level] = term if grad_radial[level] is None else grad_radial[level] + term
                spin = weighted * first
                turns[m] = spin if turns[m] is None else turns[m] + spin
            high, rest = split(grad_first)
            drows[low : low + 16, lanes] = high
            dlow[low : low + 16, lanes] = rest
            for level in range(3):
                drad[CH * level + low : CH * level + low + 16, lanes] = grad_radial[level]
        dharm[:, lanes] = jnp.concatenate(
            [jnp.sum(turns[m], 0, keepdims=True) for m in range(1, 9)], 0
        )
        return carry

    lax.fori_loop(0, SLOTS, backward, 0)

    def lane_z(dx, dy, dz):
        return slot_of(dx, dy, dz) - (2 if (dx, dy) == (0, 0) else PAIR0 // SEND - 2)

    def lane_x(dx, dy):
        return 3 * (dx > 0) + dy + 1

    def back(sends, recvs, lane, slot, chunk, go):
        part = piece(chunk)
        return remote(
            sends.at[lane, part],
            recvs.at[lane, part],
            bsend_sem,
            brecv_sem,
            CHUNKS * slot + chunk,
            go,
        )

    def back_z(dx, dy, dz, chunk):
        lane = lane_z(dx, dy, dz)
        return back(zsend, zrecv, lane, slot_of(dx, dy, dz), chunk, (0, 0, dz))

    def back_x(dx, dy, chunk):
        return back(xsend, xrecv, lane_x(dx, dy), slot_of(dx, dy, 0), chunk, (dx, 0, 0))

    def back_y(dy, chunk):
        return back(ysend, yrecv, 1 * (dy > 0), slot_of(0, dy, 0), chunk, (0, dy, 0))

    def back_place(axis, side):
        at = 1 * (side > 0)
        if axis == 2:
            source, target, go = pgrad.at[1 + at], pzrecv.at[at], (0, 0, side)
        elif axis == 0:
            source, target, go = pxsend.at[at], pxrecv.at[at], (side, 0, 0)
        else:
            source, target, go = pysend.at[at], pyrecv.at[at], (0, side, 0)
        return remote(source, target, psend_sem, precv_sem, 6 + 2 * axis + at, go)

    def folded(pair):
        return [
            jnp.concatenate(
                [pair[0:HALF, SEND * part : SEND * part + SEND], pair[HALF:FEAT, SEND * part : SEND * part + SEND]],
                1,
            )
            for part in range(2)
        ]

    def make_pairs(rank):
        row = PAIR0 + 128 * rank
        rows = dot(drows[...], onehot[row : row + 256, :], NT)
        for at in range(2):
            for dz, value in zip((-1, 1), folded(rows[:, 128 * at : 128 * at + 128])):
                zsend[lane_z(*ORDER[rank + at], dz)] = value.astype(BF16)

    def start_pairs(rank):
        for chunk in range(CHUNKS):
            for dx, dy in ORDER[rank : rank + 2]:
                for dz in (-1, 1):
                    start(back_z(dx, dy, dz, chunk))

    def keep_flats(rank):
        rows = dot(drows[...], onehot[FLAT0 + SEND * rank : FLAT0 + SEND * rank + 256, :], NT)
        for at in range(2):
            for part, value in enumerate(folded(rows[:, 128 * at : 128 * at + 128])):
                flat_g[rank + 2 * at + part] = value

    def arrived_z(dx, dy, chunk):
        rows = slice(PIECE * chunk, PIECE * chunk + PIECE)
        total = None
        for dz in (-1, 1):
            back_z(dx, dy, dz, chunk).wait_recv()
            value = zrecv[lane_z(dx, dy, dz), rows, :].astype(F32)
            total = value if total is None else total + value
        if (dx, dy) == (0, 0):
            return total
        return total + flat_g[ORDER.index((dx, dy)), rows, :]

    def arrived_x(dy, chunk):
        rows = slice(PIECE * chunk, PIECE * chunk + PIECE)
        total = arrived_z(0, dy, chunk)
        for dx in (-1, 1):
            back_x(dx, dy, chunk).wait_recv()
            total = total + xrecv[lane_x(dx, dy), rows, :].astype(F32)
        return total

    def send_x(rank):
        for chunk in range(CHUNKS):
            rows = slice(PIECE * chunk, PIECE * chunk + PIECE)
            for dx, dy in ORDER[rank : rank + 2]:
                xsend[lane_x(dx, dy), rows, :] = arrived_z(dx, dy, chunk).astype(BF16)
                start(back_x(dx, dy, chunk))

    def send_y(chunk):
        rows = slice(PIECE * chunk, PIECE * chunk + PIECE)
        for dy in (-1, 1):
            ysend[1 * (dy > 0), rows, :] = arrived_x(dy, chunk).astype(BF16)
            start(back_y(dy, chunk))

    drain()
    make_pairs(4)
    start_pairs(4)
    make_pairs(6)
    start_pairs(6)
    keep_flats(4)
    make_pairs(0)
    keep_flats(0)
    make_pairs(2)
    drain()
    start_pairs(0)
    start_pairs(2)
    send_x(4)
    send_x(6)

    before = pre[...]
    sigmoid = 1.0 / (1.0 + jnp.exp(-before))
    grad_hidden = dot(rout_ref[...], drad[...], NN, HIGH)
    grad_before = grad_hidden * (sigmoid * (1.0 + before * (1.0 - sigmoid)))
    grad_basis = dot(rin_ref[...], grad_before, NN, HIGH)
    grad_radius = jnp.sum(-(grad_basis * basis_ref[...]), 0, keepdims=True)
    displace = placed[...] + base[...]
    comp = [displace[axis : axis + 1] for axis in range(3)]
    radius = jnp.sqrt(comp[0] * comp[0] + comp[1] * comp[1] + comp[2] * comp[2] + 1.0)
    inverse = 1.0 / radius
    ux, uy, uz = (each * inverse for each in comp)
    dy1, dy2, dy3, dy4, dy5, dy6, dy7, dy8 = (dharm[m : m + 1, :] for m in range(8))
    grad_ux = ROOT_THREE * dy1 + ROOT_FIFTEEN * (uy * dy4 + uz * dy7 + ux * dy8) - ROOT_FIVE * ux * dy6
    grad_uy = ROOT_THREE * dy2 + ROOT_FIFTEEN * (ux * dy4 + uz * dy5 - uy * dy8) - ROOT_FIVE * uy * dy6
    grad_uz = ROOT_THREE * dy3 + ROOT_FIFTEEN * (uy * dy5 + ux * dy7) + 2.0 * ROOT_FIVE * uz * dy6
    along = ux * grad_ux + uy * grad_uy + uz * grad_uz
    grad_displace = jnp.concatenate(
        [
            (grad - unit * along) * inverse + grad_radius * unit
            for grad, unit in ((grad_ux, ux), (grad_uy, uy), (grad_uz, uz))
        ],
        0,
    )
    moved = grad_displace[:, 0:ATOMS]
    for slot in range(1, SLOTS):
        moved = moved + grad_displace[:, ATOMS * slot : ATOMS * slot + ATOMS]
    pieces = parts(grad_displace)
    where = blocks[0:1, :]
    for slot in range(BLOCKS):
        masked[16 * slot : 16 * slot + 16, :] = jnp.where(where == slot, pieces, 0.0).astype(BF16)
    drawn = dot(masked[...], inner[...], NT)
    own_place = joined(jnp.concatenate([drawn[0:16], drawn[16:32]], 1))
    blank = jnp.zeros((8, SEND), F32)
    pgrad[0, 4] = jnp.zeros((8, ATOMS), F32)
    for dx in (-1, 0, 1):
        for dy in (-1, 0, 1):
            for dz in (-1, 0, 1):
                if (dx, dy, dz) != (0, 0, 0):
                    slot = slot_of(dx, dy, dz)
                    pgrad[0 if dz == 0 else 1 + (dz > 0), column(dx, dy)] = jnp.concatenate(
                        [joined(drawn[16 * slot : 16 * slot + 16]), blank], 1
                    )
    for side in (-1, 1):
        start(back_place(2, side))

    rows = dot(drows[...], onehot[0:FLAT0, :], NT)
    own_g[...] = rows[:, 0:ATOMS] + dot(dlow[...], onehot[0:ATOMS, :], NT)
    for dz, value in zip((-1, 1), folded(rows[:, ATOMS:FLAT0])):
        zsend[lane_z(0, 0, dz)] = value.astype(BF16)
        for chunk in range(CHUNKS):
            start(back_z(0, 0, dz, chunk))

    for chunk in range(CHUNKS - 1):
        send_y(chunk)
    if CHUNKS == 1:
        send_x(2)
    for side in (-1, 1):
        back_place(2, side).wait_recv()
    for side in (-1, 1):
        lines = pl.ds(3 + 3 * side, 3)
        pxsend[1 * (side > 0)] = pgrad[0, lines] + pzrecv[0, lines] + pzrecv[1, lines]
        start(back_place(0, side))
    send_y(CHUNKS - 1)
    if CHUNKS > 1:
        send_x(2)
    for side in (-1, 1):
        back_place(0, side).wait_recv()
    middle = pl.ds(3, 3)
    totals = pgrad[0, middle] + pzrecv[0, middle] + pzrecv[1, middle] + pxrecv[0] + pxrecv[1]
    pysend[0] = totals[0]
    pysend[1] = totals[2]
    for side in (-1, 1):
        start(back_place(1, side))
    for chunk in range(CHUNKS):
        total = arrived_x(0, chunk)
        for dy in (-1, 1):
            back_y(dy, chunk).wait_recv()
            total = total + yrecv[1 * (dy > 0), PIECE * chunk : PIECE * chunk + PIECE, :].astype(F32)
        high, rest = split(total)
        for part, chosen in enumerate((picks_left, picks_right)):
            at = HALF * part + PIECE * chunk
            owned_ref[at : at + PIECE, :] = (
                own_g[at : at + PIECE, :] + dot(high, chosen, NT) + dot(rest, chosen, NT)
            )

    final = totals[1]
    for side in (-1, 1):
        back_place(1, side).wait_recv()
        final = final + pyrecv[1 * (side > 0)]
    force = moved - own_place[0:3] - joined(dot(parts(final).astype(BF16), picks_left, NT))[0:3]
    for axis in range(3):
        force_ref[axis] = force[axis : axis + 1]
    for copy in started:
        copy.wait_send()


def finish(energy_in, force_in, owned_in, mix_ref, energy_ref, force_ref, fgrad_ref):
    energy_ref[...] = energy_in[...]
    force_ref[...] = force_in[...]
    mix = mixers(mix_ref)
    for tile in range(4):
        rows = slice(128 * tile, 128 * tile + 128)
        high, rest = split(owned_in[rows, :])
        fgrad_ref[rows, :] = dot(mix[tile], high) + dot(mix[tile], rest)
    high, rest = split(owned_in[512:FEAT, :])
    fgrad_ref[512:FEAT, :] = dot(mix_ref[2], high) + dot(mix_ref[2], rest)


def shards(
    positions, features, species, neighbours, send_list, mix_weight, radial_in, radial_out, readout
):
    vmem = pl.BlockSpec(memory_space=pltpu.VMEM)
    results = (
        jax.ShapeDtypeStruct((1, ATOMS), F32),
        jax.ShapeDtypeStruct((3, 1, ATOMS), F32),
        jax.ShapeDtypeStruct((FEAT, ATOMS), F32),
    )
    arguments = (
        positions.reshape(3, 1, ATOMS),
        features[0, 0, 0].T,
        species[0, 0],
        neighbours.reshape(SLOTS, 1, ATOMS),
        send_list[0, 0],
        mix_weight,
        radial_in,
        radial_out,
        jnp.transpose(readout, (1, 0, 2)),
    )
    energy, forces, owned = pl.pallas_call(
        kernel,
        out_shape=results,
        in_specs=[pl.BlockSpec(memory_space=pltpu.HBM)] * 9,
        out_specs=(vmem, vmem, vmem),
        scratch_shapes=[pltpu.VMEM(each.shape, each.dtype) for each in arguments]
        + [
            pltpu.VMEM((HALF, 128), BF16),
            pltpu.VMEM((BLOCKS, HALF, 128), BF16),
            pltpu.VMEM((3, 9, 8, 128), F32),
            pltpu.VMEM((FEAT, ROWS), BF16),
            pltpu.VMEM((16 * BLOCKS, 128), BF16),
            pltpu.VMEM((ROWS, EDGES), BF16),
            pltpu.VMEM((SEND, EDGES), BF16),
            pltpu.VMEM((8, EDGES), jnp.int32),
            pltpu.VMEM((FEAT, EDGES), F32),
            pltpu.VMEM((FEAT, EDGES), BF16),
            pltpu.VMEM((8, EDGES), F32),
            pltpu.VMEM((8, EDGES), F32),
            pltpu.VMEM((SLOTS, ATOMS), jnp.int32),
            pltpu.VMEM((3 * CH, EDGES), F32),
            pltpu.VMEM((CH, EDGES), F32),
            pltpu.VMEM((8, EDGES), F32),
            pltpu.VMEM((8, EDGES), F32),
            pltpu.VMEM((FEAT, ATOMS), F32),
            pltpu.VMEM((FEAT, EDGES), BF16),
            pltpu.VMEM((FEAT, EDGES), BF16),
            pltpu.VMEM((3 * CH, EDGES), F32),
            pltpu.VMEM((8, EDGES), F32),
            pltpu.VMEM((16 * BLOCKS, EDGES), BF16),
            pltpu.VMEM((FEAT, ATOMS), F32),
            pltpu.VMEM((8, HALF, 128), F32),
            pltpu.VMEM((18, HALF, 128), BF16),
            pltpu.VMEM((18, HALF, 128), BF16),
            pltpu.VMEM((6, HALF, 128), BF16),
            pltpu.VMEM((6, HALF, 128), BF16),
            pltpu.VMEM((2, HALF, 128), BF16),
            pltpu.VMEM((2, HALF, 128), BF16),
            pltpu.VMEM((3, 9, 8, 128), F32),
            pltpu.VMEM((2, 9, 8, 128), F32),
            pltpu.VMEM((2, 3, 8, 128), F32),
            pltpu.VMEM((2, 3, 8, 128), F32),
            pltpu.VMEM((2, 8, 128), F32),
            pltpu.VMEM((2, 8, 128), F32),
            pltpu.SemaphoreType.DMA((CHUNKS * BLOCKS,)),
            pltpu.SemaphoreType.DMA((CHUNKS * BLOCKS,)),
            pltpu.SemaphoreType.DMA((CHUNKS * BLOCKS,)),
            pltpu.SemaphoreType.DMA((CHUNKS * BLOCKS,)),
            pltpu.SemaphoreType.DMA((12,)),
            pltpu.SemaphoreType.DMA((12,)),
            pltpu.SemaphoreType.DMA((9,)),
        ],
        compiler_params=pltpu.CompilerParams(
            collective_id=0, has_side_effects=True, vmem_limit_bytes=40 * 1024 * 1024
        ),
        name="layer",
    )(*[pltpu.with_memory_space_constraint(each, pltpu.HBM) for each in arguments])
    energy, forces, feature_grad = pl.pallas_call(
        finish,
        out_shape=results,
        in_specs=[vmem] * 4,
        out_specs=(vmem, vmem, vmem),
        compiler_params=pltpu.CompilerParams(vmem_limit_bytes=4 * 1024 * 1024),
        name="finish",
    )(energy, forces, owned, mix_weight)
    return (
        energy[None, None],
        forces.reshape(1, 1, 1, 3, ATOMS),
        feature_grad.T[None, None, None],
    )


def solution(mesh):
    in_specs = (
        P("gx", "gy", "gz", None, None),
        P("gx", "gy", "gz", None, None),
        P("gx", "gy", "gz", None),
        P("gx", "gy", "gz", None, None),
        P("gx", "gy", "gz", None),
        P(),
        P(),
        P(),
        P(),
    )
    out_specs = (
        P("gx", "gy", "gz", None),
        P("gx", "gy", "gz", None, None),
        P("gx", "gy", "gz", None, None),
    )
    return jax.shard_map(shards, mesh=mesh, in_specs=in_specs, out_specs=out_specs, check_vma=False)
```
